512 devices in a mesh: grp: 8 (over y), row: 64 (over z, x, core).
Axes of the slice: x: 4, y: 8, z: 8, core: 2. Of those that a mesh axis runs over, the one named last changes fastest.
Arguments:
- right_side: float32 [64, 65536], P(None, ('grp', 'row')), may hold values from -60 to 60
- links: int32 [8, 65536], P(None, ('grp', 'row')), may hold values from 0 to 65535, as said below
- coefs: float32 [65536], P(('grp', 'row')), may hold values from 0.3 to 3
- reaction: float32 [65536], P(('grp', 'row')), may hold values from 0.05 to 0.5
Outputs:
- solution: float32 [64, 65536], P(None, ('grp', 'row'))
- resid_rms: float32 [2, 64], replicated
The draws below stay inside these ranges and needn't reach their ends.
Inputs may be any that keep to these rules, and one draw needn't show every extreme that they name: `links`: the nodes form a periodic grid of 32 x 128 x 16. Block (p, q), p < 8, q < 64, holds the nodes of first coordinate p * 4 to p * 4 + 3 and second coordinate q * 2 to q * 2 + 1, and these carry the unknowns and elements b * 4 * 2 * 16 to (b + 1) * 4 * 2 * 16 - 1, with b = p * 64 + q. Element b * 4 * 2 * 16 + (i * 2 + j) * 16 + k has its base at the node (p * 4 + i, q * 2 + j, k), and its corner l lies at the base plus (l mod 2, l // 2 mod 2, l // 4), modulo the grid. Within a block the unknowns are numbered in some order. Every unknown is a corner of 8 elements.
All inputs are finite; a program needn't handle non-finite values.
Results may differ from the reference program's by a relative error of at most 0.0003.
Values sent between devices are 32-bit elements; how exact they have to be, the bound alone decides.
No kernel may reach another device: no remote copies, remote signals or barrier semaphores. Data moves between devices by JAX's collectives and lax.ppermute only.
A program may use at most 64 MiB of HBM per device.

```python
import math
import jax
import jax.numpy as jnp
import numpy as np
from jax import lax

CX = 4
CY = 2
CZ = 16
NRHS = 64
SWEEPS = 2
DEGREE = 4
NX = 32
NY = 128
NDOF = 65536
ELEMS = 65536


def draw_right_side(key, part):
    key_noise = jax.random.fold_in(key, 11)
    block_size = CX * CY * CZ
    block_count = NDOF // block_size
    position = (jnp.arange(NDOF) // block_size).astype(jnp.float32)
    rising = 1.0 + 2.0 * position / max(block_count - 1, 1)
    noise = jnp.clip(jax.random.normal(key_noise, (NRHS, NDOF), jnp.float32), -5.0, 5.0)
    return noise * rising


def draw_links(key, part):
    block_size = CX * CY * CZ
    block_count = NDOF // block_size
    row_blocks = NY // CY
    block_keys = jax.vmap(lambda number: jax.random.fold_in(key, number))(jnp.arange(block_count))
    orders = jax.vmap(lambda subkey: jax.random.permutation(subkey, block_size))(block_keys)
    element = jnp.arange(NDOF)
    owner = element // block_size
    inside = element % block_size
    first_block = owner // row_blocks
    second_block = owner % row_blocks
    first_pos = inside // (CY * CZ)
    second_pos = inside // CZ % CY
    third_pos = inside % CZ
    columns = []
    for corner in range(8):
        first = (first_block * CX + first_pos + corner % 2) % NX
        second = (second_block * CY + second_pos + corner // 2 % 2) % NY
        third = (third_pos + corner // 4) % CZ
        target = first // CX * row_blocks + second // CY
        spot = (first % CX * CY + second % CY) * CZ + third
        columns.append(target * block_size + orders[target, spot])
    return jnp.stack(columns, axis=0).astype(jnp.int32)


def levels(own_key, extent, cuts, least, top_value):
    def one(dim, parts):
        heights = jax.random.uniform(jax.random.fold_in(jax.random.fold_in(own_key, 6), dim), (parts,), jnp.float32, least / len(cuts), top_value / len(cuts))
        return jnp.repeat(jnp.exp(heights), extent[dim] // parts).reshape((-1,) + (1,) * (len(extent) - dim - 1))

    loudness = one(*cuts[0])
    for cut in cuts[1:]:
        loudness = loudness * one(*cut)
    return loudness


def setup_inputs(seed: int = 0) -> dict:
    streams_of = jax.random.split(jax.random.key(seed), 5)
    return {
        "right_side": draw_right_side(jax.random.fold_in(streams_of[4], 71), 0),
        "links": draw_links(jax.random.fold_in(streams_of[4], 71), 0),
        "coefs": jnp.clip(jnp.exp(math.log(3.0) - 2.3025851 * jax.random.uniform(streams_of[2], (ELEMS,), jnp.float32) ** levels(streams_of[2], (ELEMS,), ((0, 512),), -0.2, 0.2)), 0.3, 3.0),
        "reaction": jnp.clip(jnp.exp(math.log(0.5) - 2.3025851 * jax.random.uniform(streams_of[3], (NDOF,), jnp.float32) ** levels(streams_of[3], (NDOF,), ((0, 512),), -0.2, 0.2)), 0.05, 0.5),
    }


def element_matrix():
    node_ids = np.arange(8)
    corner = np.stack([node_ids % 2, node_ids // 2 % 2, node_ids // 4], axis=1)
    gauss_points = np.array([0.5 - 0.5 / math.sqrt(3.0), 0.5 + 0.5 / math.sqrt(3.0)])
    stiffness = np.zeros((8, 8))
    for q in range(8):
        quad_point = gauss_points[np.array([q % 2, q // 2 % 2, q // 4])]
        values = np.where(corner > 0.5, quad_point, 1.0 - quad_point)
        slopes = np.where(corner > 0.5, 1.0, -1.0)
        gradient = np.stack([slopes[:, 0] * values[:, 1] * values[:, 2], values[:, 0] * slopes[:, 1] * values[:, 2], values[:, 0] * values[:, 1] * slopes[:, 2]], axis=1)
        stiffness = stiffness + gradient @ gradient.T / 8.0
    return stiffness

def apply_operator(field, links, coefs, reaction, stiffness):
    corners = field[:, links]
    images = jnp.einsum('ml,rle->rme', stiffness, corners, precision=lax.Precision.HIGHEST) * coefs
    result = reaction * field
    return result.at[:, links].add(images)

def reference(right_side, links, coefs, reaction):
    stiffness = jnp.asarray(element_matrix(), dtype=jnp.float32)
    image = apply_operator(right_side, links, coefs, reaction, stiffness)
    theta = lax.optimization_barrier(jnp.sum(image * image, axis=1)) / lax.optimization_barrier(jnp.sum(right_side * image, axis=1))
    upper = (1.5 * theta)[:, None]
    lower = upper / 10.0
    center = (upper + lower) / 2.0
    half = (upper - lower) / 2.0
    sigma = center / half
    solution = jnp.zeros_like(right_side)
    residual = right_side
    history = []
    for sweep in range(SWEEPS):
        start = residual
        correction = jnp.zeros_like(right_side)
        rho_now = 1.0 / sigma
        direction = residual / center
        for step in range(DEGREE):
            correction = correction + direction
            residual = residual - apply_operator(direction, links, coefs, reaction, stiffness)
            if step + 1 < DEGREE:
                rho_next = 1.0 / (2.0 * sigma - rho_now)
                direction = rho_next * rho_now * direction + 2.0 * rho_next / half * residual
                rho_now = rho_next
        change = start - residual
        omega = (lax.optimization_barrier(jnp.sum(start * change, axis=1)) / lax.optimization_barrier(jnp.sum(change * change, axis=1)))[:, None]
        solution = solution + omega * correction
        residual = start - omega * change
        history.append(jnp.sqrt(lax.optimization_barrier(jnp.sum(residual * residual, axis=1)) / NDOF))
    return (solution, jnp.stack(history, axis=0))
```

```python
import jax
import jax.numpy as jnp
from jax import lax
from jax.experimental import pallas as pl
from jax.experimental.pallas import tpu as pltpu
from jax.sharding import Mesh
from jax.sharding import PartitionSpec as P

SWEEPS = 2
DEGREE = 4
HIGHEST = lax.Precision.HIGHEST


def dot(a, b, dims=((1,), (0,))):
    return lax.dot_general(a, b, (dims, ((), ())), precision=HIGHEST, preferred_element_type=jnp.float32)


def pack_kernel(right_ref, links_ref, coefs_ref, reaction_ref, message_ref, order_ref):
    row = lax.broadcasted_iota(jnp.int32, (128, 128), 0)
    lane = lax.broadcasted_iota(jnp.int32, (128, 128), 1)
    regroup = (row == (lane % 8) * 16 + lane // 8).astype(jnp.float32)
    slot = links_ref[0:1, :] & 127
    onehot = (row == slot).astype(jnp.float32)
    order = dot(onehot, regroup)
    order_ref[...] = order
    message_ref[:, 0:128] = dot(right_ref[...], order)
    coefs = dot(jnp.broadcast_to(coefs_ref[...], (8, 128)), regroup)
    reaction = dot(jnp.broadcast_to(reaction_ref[...], (8, 128)), order)
    for block in range(8):
        message_ref[block * 8 : block * 8 + 8, 128:256] = coefs
        message_ref[block * 8 : block * 8 + 8, 256:384] = reaction


def unpack_kernel(message_ref, order_ref, solution_ref, history_ref):
    solution_ref[...] = dot(message_ref[:, 0:128], order_ref[...], ((1,), (1,)))
    history_ref[...] = jnp.transpose(message_ref[:, 128:256])[0:8, :]


def exchange_lanes(tile):
    row = lax.broadcasted_iota(jnp.int32, (8, 128), 0)
    lane = lax.broadcasted_iota(jnp.int32, (8, 128), 1)
    for bit in (1, 2, 4):
        from_below = pltpu.roll(pltpu.roll(tile, 8 - bit, 0), bit, 1)
        from_above = pltpu.roll(pltpu.roll(tile, bit, 0), 128 - bit, 1)
        lane_bit = (lane & bit) != 0
        same = ((row & bit) != 0) == lane_bit
        tile = jnp.where(same, tile, jnp.where(lane_bit, from_below, from_above))
    return tile


def solve_kernel(
    parts_ref, out_ref, regroup_ref, shift_ref, direct_ref, turned_ref, residual_ref, start_ref,
    coef_ref, reaction_ref, minus_ref, plus_ref, correct_ref, solution_ref,
):
    lane = lax.broadcasted_iota(jnp.int32, (8, 128), 1)
    last_z = (lane & 7) == 7
    first_z = (lane & 7) == 0
    mine = lax.axis_index("x") * 2 + lax.axis_index("core")

    def next_z(v):
        return jnp.where(last_z, pltpu.roll(v, 7, 1), pltpu.roll(v, 127, 1))

    def prev_z(v):
        return jnp.where(first_z, pltpu.roll(v, 121, 1), pltpu.roll(v, 1, 1))

    def next_k(v):
        return pltpu.roll(v, 120, 1)

    def prev_k(v):
        return pltpu.roll(v, 8, 1)

    cells = [(i, w) for w in range(16) for i in range(4)]

    for kind in range(3):
        for x in range(4):
            for core in range(2):
                for y in range(8):
                    tile = parts_ref[core, x, y * 8 : y * 8 + 8, kind * 128 : kind * 128 + 128]
                    regroup_ref[x * 2 + core, y * 8 : y * 8 + 8, :] = exchange_lanes(tile)
        for i, w in cells:
            v = regroup_ref[w // 2, pl.ds(i * 2 + w % 2, 8, stride=8), :]
            if kind == 0:
                residual_ref[i, w] = v
                direct_ref[i, w] = v
                turned_ref[i, w] = next_k(v)
            elif kind == 1:
                coef_ref[0, i, w] = v * (1.0 / 16.0)
                coef_ref[1, i, w] = v * (1.0 / 24.0)
                coef_ref[2, i, w] = v * (1.0 / 48.0)
            else:
                reaction_ref[i, w] = v

    def halves(v, shifted):
        return v + shifted, shifted - v

    def next_i(vs):
        return [vs[1], vs[2], vs[3], pltpu.roll(vs[0], 7, 0)]

    def prev_i(vs):
        return [pltpu.roll(vs[3], 1, 0), vs[0], vs[1], vs[2]]

    def fold(minus_sum, sums):
        return [m + s for m, s in zip(minus_sum, prev_i(sums))]

    def apply_stiffness():
        def load(w):
            pairs = [halves(direct_ref[i, w], turned_ref[i, w]) for i in range(4)]
            return [p[0] for p in pairs], [p[1] for p in pairs]

        wrapped = []
        for i in range(4):
            v = next_z(direct_ref[i, 0])
            wrapped.append(halves(v, next_k(v)))
        wrapped = [p[0] for p in wrapped], [p[1] for p in wrapped]
        here = load(0)
        carry = None
        kept = None
        for w in range(16):
            there = load(w + 1) if w < 15 else wrapped
            grads = []
            for zk in range(2):
                for yk in range(2):
                    vs = [halves(a, b)[yk] for a, b in zip(here[zk], there[zk])]
                    nexts = next_i(vs)
                    differ = [(b - a) * coef_ref[zk + yk, i, w] for i, (a, b) in enumerate(zip(vs, nexts))]
                    if zk + yk:
                        total = [(a + b) * coef_ref[zk + yk - 1, i, w] for i, (a, b) in enumerate(zip(vs, nexts))]
                        grads.append(fold([s - d for s, d in zip(total, differ)], [s + d for s, d in zip(total, differ)]))
                    else:
                        grads.append(fold([-d for d in differ], differ))
            low = [[s - d for s, d in zip(grads[zk * 2], grads[zk * 2 + 1])] for zk in range(2)]
            high = [[s + d for s, d in zip(grads[zk * 2], grads[zk * 2 + 1])] for zk in range(2)]
            if w == 0:
                kept = low
            else:
                low = [[a + b for a, b in zip(low[zk], carry[zk])] for zk in range(2)]
                for i in range(4):
                    minus_ref[i, w] = low[0][i] - low[1][i]
                    plus_ref[i, w] = low[0][i] + low[1][i]
            carry = high
            here = there
        for i in range(4):
            s = kept[0][i] + prev_z(carry[0][i])
            d = kept[1][i] + prev_z(carry[1][i])
            minus_ref[i, 0] = s - d
            plus_ref[i, 0] = s + d

    def image_of(i, w, v):
        return minus_ref[i, w] + prev_k(plus_ref[i, w]) + reaction_ref[i, w] * v

    def over_all(v):
        return jnp.sum(jnp.sum(v, axis=1, keepdims=True), axis=0, keepdims=True)

    zero = jnp.zeros((8, 128), jnp.float32)

    apply_stiffness()
    crosses = [zero] * 4
    squares = [zero] * 4
    for i, w in cells:
        v = direct_ref[i, w]
        image = image_of(i, w, v)
        crosses[i] = crosses[i] + v * image
        squares[i] = squares[i] + image * image
    cross = over_all((crosses[0] + crosses[1]) + (crosses[2] + crosses[3]))
    square = over_all((squares[0] + squares[1]) + (squares[2] + squares[3]))
    theta = square / cross
    upper = 1.5 * theta
    lower = upper / 10.0
    center = (upper + lower) / 2.0
    half = (upper - lower) / 2.0
    sigma = center / half
    per_center = 1.0 / center

    for sweep in range(SWEEPS):
        scale = jnp.broadcast_to(per_center, (8, 128))
        for i, w in cells:
            r = residual_ref[i, w]
            start_ref[i, w] = r
            v = r * scale
            direct_ref[i, w] = v
            turned_ref[i, w] = next_k(v)
        for ij in range(8):
            correct_ref[ij] = zero

        def step(_, rho_now):
            for ij in range(8):
                correct_ref[ij] = correct_ref[ij] + direct_ref[ij // 2, mine * 2 + ij % 2]
            apply_stiffness()
            rho_next = 1.0 / (2.0 * sigma - rho_now)
            along = jnp.broadcast_to(rho_next * rho_now, (8, 128))
            across = jnp.broadcast_to(2.0 * rho_next / half, (8, 128))
            for i, w in cells:
                v = direct_ref[i, w]
                r = residual_ref[i, w] - image_of(i, w, v)
                residual_ref[i, w] = r
                v = along * v + across * r
                direct_ref[i, w] = v
                turned_ref[i, w] = next_k(v)
            return rho_next

        lax.fori_loop(0, DEGREE, step, 1.0 / sigma)
        crosses = [zero] * 4
        squares = [zero] * 4
        for i, w in cells:
            s = start_ref[i, w]
            change = s - residual_ref[i, w]
            crosses[i] = crosses[i] + s * change
            squares[i] = squares[i] + change * change
        along = over_all((crosses[0] + crosses[1]) + (crosses[2] + crosses[3]))
        length = over_all((squares[0] + squares[1]) + (squares[2] + squares[3]))
        omega = jnp.broadcast_to(along / length, (8, 128))
        squares = [zero] * 4
        for i, w in cells:
            s = start_ref[i, w]
            r = s - omega * (s - residual_ref[i, w])
            residual_ref[i, w] = r
            squares[i] = squares[i] + r * r
        for ij in range(8):
            if sweep == 0:
                solution_ref[ij] = omega * correct_ref[ij]
            else:
                solution_ref[ij] = solution_ref[ij] + omega * correct_ref[ij]
        total = over_all((squares[0] + squares[1]) + (squares[2] + squares[3]))
        rms = jnp.broadcast_to(jnp.sqrt(total / 65536.0), (8, 128))
        if sweep == 0:
            history = rms
        else:
            history = jnp.where(lane == sweep, rms, history)

    for ij in range(8):
        shift_ref[pl.ds(ij, 8, stride=8), :] = solution_ref[ij]
    for y in range(8):
        out_ref[y * 8 : y * 8 + 8, 0:128] = exchange_lanes(shift_ref[y * 8 : y * 8 + 8, :])
        out_ref[y * 8 : y * 8 + 8, 128:256] = history


def field(*lead):
    return pltpu.VMEM((*lead, 8, 128), jnp.float32)


def solve(parts):
    whole = field(4, 16)
    return pl.pallas_call(
        solve_kernel,
        out_shape=jax.ShapeDtypeStruct((64, 256), jnp.float32),
        scratch_shapes=[
            pltpu.VMEM((8, 64, 128), jnp.float32), pltpu.VMEM((64, 128), jnp.float32),
            whole, whole, whole, whole, field(3, 4, 16), whole, whole, whole, field(8), field(8),
        ],
        compiler_params=pltpu.CompilerParams(vmem_limit_bytes=40 * 1024 * 1024),
        name="solve",
    )(parts)


def on_device(right_side, links, coefs, reaction):
    message, order = pl.pallas_call(
        pack_kernel,
        out_shape=(jax.ShapeDtypeStruct((64, 384), jnp.float32), jax.ShapeDtypeStruct((128, 128), jnp.float32)),
        name="pack",
    )(right_side, links, coefs.reshape(1, 128), reaction.reshape(1, 128))
    received = lax.all_to_all(message, ("grp", "z"), 0, 0, tiled=True)
    along_x = lax.all_to_all(jnp.broadcast_to(received[None], (4, 64, 384)), "x", 0, 0, tiled=True)
    parts = lax.all_gather(along_x, "core", axis=0)
    answer = solve(parts)
    answer = lax.all_to_all(answer, ("grp", "z"), 0, 0, tiled=True)
    result, history = pl.pallas_call(
        unpack_kernel,
        out_shape=(jax.ShapeDtypeStruct((64, 128), jnp.float32), jax.ShapeDtypeStruct((8, 64), jnp.float32)),
        name="unpack",
    )(answer, order)
    return result, history[0:SWEEPS]


def solution(mesh):
    finer = Mesh(mesh.devices.reshape(8, 8, 4, 2), ("grp", "z", "x", "core"))
    blocks = ("grp", "z", "x", "core")
    return jax.shard_map(
        on_device,
        mesh=finer,
        in_specs=(P(None, blocks), P(None, blocks), P(blocks), P(blocks)),
        out_specs=(P(None, blocks), P()),
        check_vma=False,
    )
```

```python
import jax
import jax.numpy as jnp
from jax import lax
from jax.experimental import pallas as pl
from jax.experimental.pallas import tpu as pltpu
from jax.sharding import Mesh
from jax.sharding import PartitionSpec as P

SWEEPS = 2
DEGREE = 4
HIGHEST = lax.Precision.HIGHEST
SMALL = pltpu.CompilerParams(vmem_limit_bytes=16 * 1024 * 1024)


def dot(a, b, dims=((1,), (0,))):
    return lax.dot_general(a, b, (dims, ((), ())), precision=HIGHEST, preferred_element_type=jnp.float32)


def orders_of(links_ref):
    row = lax.broadcasted_iota(jnp.int32, (128, 128), 0)
    lane = lax.broadcasted_iota(jnp.int32, (128, 128), 1)
    regroup = (row == (lane % 8) * 16 + lane // 8).astype(jnp.bfloat16)
    onehot = (row == (links_ref[0:1, :] & 127)).astype(jnp.bfloat16)
    order = jnp.dot(onehot, regroup, preferred_element_type=jnp.float32)
    return regroup.astype(jnp.float32), order


def pack_kernel(right_hbm, links_hbm, coefs_hbm, reaction_hbm, message_ref, order_ref, right_ref, links_ref, coefs_ref, reaction_ref, semaphores):
    copies = [
        pltpu.make_async_copy(source, target, semaphores.at[n])
        for n, (source, target) in enumerate(
            [(links_hbm, links_ref), (right_hbm, right_ref), (coefs_hbm, coefs_ref), (reaction_hbm, reaction_ref)]
        )
    ]
    for copy in copies:
        copy.start()
    copies[0].wait()
    regroup, order = orders_of(links_ref)
    order_ref[...] = order
    for copy in copies[1:]:
        copy.wait()
    message_ref[:, 0:128] = dot(right_ref[...], order)
    coefs = dot(jnp.broadcast_to(coefs_ref[...], (8, 128)), regroup)
    reaction = dot(jnp.broadcast_to(reaction_ref[...], (8, 128)), order)
    for block in range(8):
        message_ref[block * 8 : block * 8 + 8, 128:256] = coefs
        message_ref[block * 8 : block * 8 + 8, 256:384] = reaction


def unpack_kernel(message_ref, order_ref, solution_ref, history_ref):
    solution_ref[...] = dot(message_ref[:, 0:128], order_ref[...], ((1,), (1,)))
    history_ref[...] = jnp.transpose(message_ref[:, 128:256])[0:SWEEPS, :]


def exchange_lanes(tile):
    row = lax.broadcasted_iota(jnp.int32, (8, 128), 0)
    lane = lax.broadcasted_iota(jnp.int32, (8, 128), 1)
    for bit in (1, 2, 4):
        from_below = pltpu.roll(pltpu.roll(tile, 8 - bit, 0), bit, 1)
        from_above = pltpu.roll(pltpu.roll(tile, bit, 0), 128 - bit, 1)
        lane_bit = (lane & bit) != 0
        same = ((row & bit) != 0) == lane_bit
        tile = jnp.where(same, tile, jnp.where(lane_bit, from_below, from_above))
    return tile


def exchange_rows(tiles):
    row = lax.broadcasted_iota(jnp.int32, (8, 128), 0)
    tiles = list(tiles)
    for bit in (1, 2, 4):
        upper = (row & bit) != 0
        for a in range(8):
            if not a & bit:
                b = a | bit
                first, second = tiles[a], tiles[b]
                tiles[a] = jnp.where(upper, pltpu.roll(second, bit, 0), first)
                tiles[b] = jnp.where(upper, second, pltpu.roll(first, 8 - bit, 0))
    return tiles


def spread_kernel(message_ref, out_ref):
    for kind in range(3):
        tiles = [
            exchange_lanes(message_ref[y * 8 : y * 8 + 8, kind * 128 : kind * 128 + 128]) for y in range(8)
        ]
        for ij, tile in enumerate(exchange_rows(tiles)):
            for x in range(4):
                out_ref[x, kind, ij] = tile


def solve_kernel(
    parts_ref, out_ref, direct_ref, turned_ref, residual_ref, start_ref, coef_ref, minus_ref, plus_ref,
    correct_ref, solution_ref,
):
    lane = lax.broadcasted_iota(jnp.int32, (8, 128), 1)
    last_z = (lane & 7) == 7
    first_z = (lane & 7) == 0
    mine = lax.axis_index("x") * 2 + lax.axis_index("core")

    def next_z(v):
        return jnp.where(last_z, pltpu.roll(v, 7, 1), pltpu.roll(v, 127, 1))

    def prev_z(v):
        return jnp.where(first_z, pltpu.roll(v, 121, 1), pltpu.roll(v, 1, 1))

    def next_k(v):
        return pltpu.roll(v, 120, 1)

    def prev_k(v):
        return pltpu.roll(v, 8, 1)

    cells = [(i, w) for w in range(16) for i in range(4)]

    def given(kind, i, w):
        return parts_ref[w // 2 % 2, w // 4, kind, i * 2 + w % 2]

    for i, w in cells:
        v = given(0, i, w)
        residual_ref[i, w] = v
        direct_ref[i, w] = v
        turned_ref[i, w] = next_k(v)
        c = given(1, i, w)
        coef_ref[0, i, w] = c * (1.0 / 16.0)
        coef_ref[1, i, w] = c * (1.0 / 24.0)
        coef_ref[2, i, w] = c * (1.0 / 48.0)

    def halves(v, shifted):
        return v + shifted, shifted - v

    def next_i(vs):
        return [vs[1], vs[2], vs[3], pltpu.roll(vs[0], 7, 0)]

    def prev_i(vs):
        return [pltpu.roll(vs[3], 1, 0), vs[0], vs[1], vs[2]]

    def fold(minus_sum, sums):
        return [m + s for m, s in zip(minus_sum, prev_i(sums))]

    def apply_stiffness():
        def load(w):
            pairs = [halves(direct_ref[i, w], turned_ref[i, w]) for i in range(4)]
            return [p[0] for p in pairs], [p[1] for p in pairs]

        wrapped = []
        for i in range(4):
            v = next_z(direct_ref[i, 0])
            wrapped.append(halves(v, next_k(v)))
        wrapped = [p[0] for p in wrapped], [p[1] for p in wrapped]
        here = load(0)
        carry = None
        kept = None
        for w in range(16):
            there = load(w + 1) if w < 15 else wrapped
            grads = []
            for zk in range(2):
                for yk in range(2):
                    vs = [halves(a, b)[yk] for a, b in zip(here[zk], there[zk])]
                    nexts = next_i(vs)
                    differ = [(b - a) * coef_ref[zk + yk, i, w] for i, (a, b) in enumerate(zip(vs, nexts))]
                    if zk + yk:
                        total = [(a + b) * coef_ref[zk + yk - 1, i, w] for i, (a, b) in enumerate(zip(vs, nexts))]
                        grads.append(fold([s - d for s, d in zip(total, differ)], [s + d for s, d in zip(total, differ)]))
                    else:
                        grads.append(fold([-d for d in differ], differ))
            low = [[s - d for s, d in zip(grads[zk * 2], grads[zk * 2 + 1])] for zk in range(2)]
            high = [[s + d for s, d in zip(grads[zk * 2], grads[zk * 2 + 1])] for zk in range(2)]
            if w == 0:
                kept = low
            else:
                low = [[a + b for a, b in zip(low[zk], carry[zk])] for zk in range(2)]
                for i in range(4):
                    minus_ref[i, w] = low[0][i] - low[1][i]
                    plus_ref[i, w] = low[0][i] + low[1][i]
            carry = high
            here = there
        for i in range(4):
            s = kept[0][i] + prev_z(carry[0][i])
            d = kept[1][i] + prev_z(carry[1][i])
            minus_ref[i, 0] = s - d
            plus_ref[i, 0] = s + d

    def image_of(i, w, v):
        return minus_ref[i, w] + prev_k(plus_ref[i, w]) + given(2, i, w) * v

    def over_all(v):
        return jnp.sum(jnp.sum(v, axis=1, keepdims=True), axis=0, keepdims=True)

    zero = jnp.zeros((8, 128), jnp.float32)

    apply_stiffness()
    crosses = [zero] * 4
    squares = [zero] * 4
    for i, w in cells:
        v = direct_ref[i, w]
        image = image_of(i, w, v)
        crosses[i] = crosses[i] + v * image
        squares[i] = squares[i] + image * image
    cross = over_all((crosses[0] + crosses[1]) + (crosses[2] + crosses[3]))
    square = over_all((squares[0] + squares[1]) + (squares[2] + squares[3]))
    theta = square / cross
    upper = 1.5 * theta
    lower = upper / 10.0
    center = (upper + lower) / 2.0
    half = (upper - lower) / 2.0
    sigma = center / half
    per_center = 1.0 / center

    for sweep in range(SWEEPS):
        scale = jnp.broadcast_to(per_center, (8, 128))
        for i, w in cells:
            r = residual_ref[i, w]
            start_ref[i, w] = r
            v = r * scale
            direct_ref[i, w] = v
            turned_ref[i, w] = next_k(v)
        for ij in range(8):
            correct_ref[ij] = zero

        def step(_, rho_now):
            for ij in range(8):
                correct_ref[ij] = correct_ref[ij] + direct_ref[ij // 2, mine * 2 + ij % 2]
            apply_stiffness()
            rho_next = 1.0 / (2.0 * sigma - rho_now)
            along = jnp.broadcast_to(rho_next * rho_now, (8, 128))
            across = jnp.broadcast_to(2.0 * rho_next / half, (8, 128))
            for i, w in cells:
                v = direct_ref[i, w]
                r = residual_ref[i, w] - image_of(i, w, v)
                residual_ref[i, w] = r
                v = along * v + across * r
                direct_ref[i, w] = v
                turned_ref[i, w] = next_k(v)
            return rho_next

        lax.fori_loop(0, DEGREE, step, 1.0 / sigma)
        crosses = [zero] * 4
        squares = [zero] * 4
        for i, w in cells:
            s = start_ref[i, w]
            change = s - residual_ref[i, w]
            crosses[i] = crosses[i] + s * change
            squares[i] = squares[i] + change * change
        along = over_all((crosses[0] + crosses[1]) + (crosses[2] + crosses[3]))
        length = over_all((squares[0] + squares[1]) + (squares[2] + squares[3]))
        omega = jnp.broadcast_to(along / length, (8, 128))
        squares = [zero] * 4
        for i, w in cells:
            s = start_ref[i, w]
            r = s - omega * (s - residual_ref[i, w])
            residual_ref[i, w] = r
            squares[i] = squares[i] + r * r
        for ij in range(8):
            if sweep == 0:
                solution_ref[ij] = omega * correct_ref[ij]
            else:
                solution_ref[ij] = solution_ref[ij] + omega * correct_ref[ij]
        total = over_all((squares[0] + squares[1]) + (squares[2] + squares[3]))
        rms = jnp.broadcast_to(jnp.sqrt(total / 65536.0), (8, 128))
        if sweep == 0:
            history = rms
        else:
            history = jnp.where(lane == sweep, rms, history)

    for y, tile in enumerate(exchange_rows([solution_ref[ij] for ij in range(8)])):
        out_ref[y * 8 : y * 8 + 8, 0:128] = exchange_lanes(tile)
        out_ref[y * 8 : y * 8 + 8, 128:256] = history


def field(*lead):
    return pltpu.VMEM((*lead, 8, 128), jnp.float32)


def solve(parts):
    whole = field(4, 16)
    return pl.pallas_call(
        solve_kernel,
        out_shape=jax.ShapeDtypeStruct((64, 256), jnp.float32),
        scratch_shapes=[
            whole, whole, whole, whole, field(3, 4, 16), whole, whole, field(8), field(8),
        ],
        compiler_params=SMALL,
        name="solve",
    )(parts)


def on_device(right_side, links, coefs, reaction):
    message, order = pl.pallas_call(
        pack_kernel,
        out_shape=(jax.ShapeDtypeStruct((64, 384), jnp.float32), jax.ShapeDtypeStruct((128, 128), jnp.float32)),
        in_specs=[pl.BlockSpec(memory_space=pltpu.HBM)] * 4,
        scratch_shapes=[
            pltpu.VMEM((64, 128), jnp.float32), pltpu.VMEM((8, 128), jnp.int32),
            pltpu.VMEM((1, 128), jnp.float32), pltpu.VMEM((1, 128), jnp.float32), pltpu.SemaphoreType.DMA((4,)),
        ],
        compiler_params=SMALL,
        name="pack",
    )(right_side, links, coefs.reshape(1, 128), reaction.reshape(1, 128))
    received = lax.all_to_all(message, ("grp", "z"), 0, 0, tiled=True)
    spread = pl.pallas_call(
        spread_kernel,
        out_shape=jax.ShapeDtypeStruct((4, 3, 8, 8, 128), jnp.float32),
        compiler_params=SMALL,
        name="spread",
    )(received)
    parts = lax.all_gather(lax.all_to_all(spread, "x", 0, 0, tiled=True), "core", axis=0)
    answer = solve(parts)
    answer = lax.all_to_all(answer, ("grp", "z"), 0, 0, tiled=True)
    return pl.pallas_call(
        unpack_kernel,
        out_shape=(jax.ShapeDtypeStruct((64, 128), jnp.float32), jax.ShapeDtypeStruct((SWEEPS, 64), jnp.float32)),
        compiler_params=SMALL,
        name="unpack",
    )(answer, order)


def solution(mesh):
    finer = Mesh(mesh.devices.reshape(8, 8, 4, 2), ("grp", "z", "x", "core"))
    blocks = ("grp", "z", "x", "core")
    return jax.shard_map(
        on_device,
        mesh=finer,
        in_specs=(P(None, blocks), P(None, blocks), P(blocks), P(blocks)),
        out_specs=(P(None, blocks), P()),
        check_vma=False,
    )
```

```python
import jax
import jax.numpy as jnp
from jax import lax
from jax.experimental import pallas as pl
from jax.experimental.pallas import tpu as pltpu
from jax.sharding import Mesh
from jax.sharding import PartitionSpec as P

SWEEPS = 2
DEGREE = 4
HIGHEST = lax.Precision.HIGHEST
SMALL = pltpu.CompilerParams(vmem_limit_bytes=16 * 1024 * 1024)


def dot(a, b, dims=((1,), (0,))):
    return lax.dot_general(a, b, (dims, ((), ())), precision=HIGHEST, preferred_element_type=jnp.float32)


def orders_of(links_ref):
    row = lax.broadcasted_iota(jnp.int32, (128, 128), 0)
    lane = lax.broadcasted_iota(jnp.int32, (128, 128), 1)
    regroup = (row == (lane % 8) * 16 + lane // 8).astype(jnp.bfloat16)
    onehot = (row == (links_ref[0:1, :] & 127)).astype(jnp.bfloat16)
    order = jnp.dot(onehot, regroup, preferred_element_type=jnp.float32)
    return regroup.astype(jnp.float32), order


def pack_kernel(right_hbm, links_hbm, coefs_hbm, reaction_hbm, message_ref, order_ref, right_ref, links_ref, coefs_ref, reaction_ref, semaphores):
    copies = [
        pltpu.make_async_copy(source, target, semaphores.at[n])
        for n, (source, target) in enumerate(
            [(links_hbm, links_ref), (right_hbm, right_ref), (coefs_hbm, coefs_ref), (reaction_hbm, reaction_ref)]
        )
    ]
    for copy in copies:
        copy.start()
    copies[0].wait()
    regroup, order = orders_of(links_ref)
    order_ref[...] = order
    for copy in copies[1:]:
        copy.wait()
    message_ref[:, 0:128] = dot(right_ref[...], order)
    coefs = dot(jnp.broadcast_to(coefs_ref[...], (8, 128)), regroup)
    reaction = dot(jnp.broadcast_to(reaction_ref[...], (8, 128)), order)
    for block in range(8):
        message_ref[block * 8 : block * 8 + 8, 128:256] = coefs
        message_ref[block * 8 : block * 8 + 8, 256:384] = reaction


def unpack_kernel(message_ref, order_ref, solution_ref, history_ref):
    solution_ref[...] = dot(message_ref[:, 0:128], order_ref[...], ((1,), (1,)))
    history_ref[...] = jnp.transpose(message_ref[:, 128:256])[0:SWEEPS, :]


def exchange_lanes(tile):
    row = lax.broadcasted_iota(jnp.int32, (8, 128), 0)
    lane = lax.broadcasted_iota(jnp.int32, (8, 128), 1)
    for bit in (1, 2, 4):
        from_below = pltpu.roll(pltpu.roll(tile, 8 - bit, 0), bit, 1)
        from_above = pltpu.roll(pltpu.roll(tile, bit, 0), 128 - bit, 1)
        lane_bit = (lane & bit) != 0
        same = ((row & bit) != 0) == lane_bit
        tile = jnp.where(same, tile, jnp.where(lane_bit, from_below, from_above))
    return tile


def exchange_rows(tiles):
    row = lax.broadcasted_iota(jnp.int32, (8, 128), 0)
    tiles = list(tiles)
    for bit in (1, 2, 4):
        upper = (row & bit) != 0
        for a in range(8):
            if not a & bit:
                b = a | bit
                first, second = tiles[a], tiles[b]
                tiles[a] = jnp.where(upper, pltpu.roll(second, bit, 0), first)
                tiles[b] = jnp.where(upper, second, pltpu.roll(first, 8 - bit, 0))
    return tiles


def spread_kernel(message_ref, out_ref):
    for kind in range(3):
        tiles = [
            exchange_lanes(message_ref[y * 8 : y * 8 + 8, kind * 128 : kind * 128 + 128]) for y in range(8)
        ]
        for ij, tile in enumerate(exchange_rows(tiles)):
            for x in range(4):
                out_ref[x, kind, ij] = tile


def solve_kernel(
    parts_ref, out_ref, direct_ref, turned_ref, residual_ref, start_ref, coef_ref,
    correct_ref, solution_ref,
):
    lane = lax.broadcasted_iota(jnp.int32, (8, 128), 1)
    last_z = (lane & 7) == 7
    first_z = (lane & 7) == 0
    mine = lax.axis_index("x") * 2 + lax.axis_index("core")

    def next_z(v):
        return jnp.where(last_z, pltpu.roll(v, 7, 1), pltpu.roll(v, 127, 1))

    def prev_z(v):
        return jnp.where(first_z, pltpu.roll(v, 121, 1), pltpu.roll(v, 1, 1))

    def next_k(v):
        return pltpu.roll(v, 120, 1)

    def prev_k(v):
        return pltpu.roll(v, 8, 1)

    cells = [(i, w) for w in range(16) for i in range(4)]

    def given(kind, i, w):
        return parts_ref[w // 2 % 2, w // 4, kind, i * 2 + w % 2]

    def next_i(vs):
        return [vs[1], vs[2], vs[3], pltpu.roll(vs[0], 7, 0)]

    def prev_i(vs):
        return [pltpu.roll(vs[3], 1, 0), vs[0], vs[1], vs[2]]

    def mul(a, b):
        return [p * q for p, q in zip(a, b)]

    def add(a, b):
        return [p + q for p, q in zip(a, b)]

    def sub(a, b):
        return [p - q for p, q in zip(a, b)]

    for w in range(16):
        below = [given(1, i, w) * (1.0 / 48.0) for i in range(4)]
        both = add(below, prev_i(below))
        for i in range(4):
            v = given(0, i, w)
            residual_ref[i, w] = v
            direct_ref[i, w] = v
            turned_ref[i, w] = next_k(v)
            coef_ref[0, i, w] = below[i]
            coef_ref[1, i, w] = below[i] * 3.0
            coef_ref[2, i, w] = both[i] * 5.0
            coef_ref[3, i, w] = both[i] * 3.0

    def apply(visit):
        def load(w):
            here = [direct_ref[i, w] for i in range(4)]
            turned = [turned_ref[i, w] for i in range(4)]
            return add(here, turned), sub(turned, here)

        def column(w, here, there):
            coef = [[coef_ref[n, i, w] for i in range(4)] for n in range(4)]
            lows, highs = [], []
            for zk in range(2):
                total, differ = add(here[zk], there[zk]), sub(there[zk], here[zk])
                if zk == 0:
                    flux = mul(coef[1], sub(next_i(total), total))
                    total = sub(prev_i(flux), flux)
                else:
                    total = couple(coef[2], coef[0], total)
                differ = couple(coef[2 + zk], coef[0], differ)
                lows.append(sub(total, differ))
                highs.append(add(total, differ))
            return lows, highs

        def couple(center, side, vs):
            return add(add(mul(center, vs), mul(side, next_i(vs))), prev_i(mul(side, vs)))

        def finish(w, totals):
            for i in range(4):
                total, differ = totals[0][i], totals[1][i]
                v = direct_ref[i, w]
                visit(i, w, v, ((total - differ) + given(2, i, w) * v) + prev_k(total + differ))

        here = load(15)
        wrapped = [next_z(direct_ref[i, 0]) for i in range(4)]
        turned = [next_k(v) for v in wrapped]
        kept, carry = column(15, here, (add(wrapped, turned), sub(turned, wrapped)))
        carry = [[prev_z(v) for v in vs] for vs in carry]
        last = here
        here = load(0)
        for w in range(15):
            there = load(w + 1) if w < 14 else last
            low, high = column(w, here, there)
            finish(w, [add(p, q) for p, q in zip(low, carry)])
            carry, here = high, there
        finish(15, [add(p, q) for p, q in zip(kept, carry)])

    def over_all(v):
        return jnp.sum(jnp.sum(v, axis=1, keepdims=True), axis=0, keepdims=True)

    zero = jnp.zeros((8, 128), jnp.float32)

    crosses = [zero] * 4
    squares = [zero] * 4

    def measure(i, w, v, image):
        crosses[i] = crosses[i] + v * image
        squares[i] = squares[i] + image * image

    apply(measure)
    cross = over_all((crosses[0] + crosses[1]) + (crosses[2] + crosses[3]))
    square = over_all((squares[0] + squares[1]) + (squares[2] + squares[3]))
    theta = square / cross
    upper = 1.5 * theta
    lower = upper / 10.0
    center = (upper + lower) / 2.0
    half = (upper - lower) / 2.0
    sigma = center / half
    per_center = 1.0 / center

    for sweep in range(SWEEPS):
        scale = jnp.broadcast_to(per_center, (8, 128))
        for i, w in cells:
            r = residual_ref[i, w]
            start_ref[i, w] = r
            v = r * scale
            direct_ref[i, w] = v
            turned_ref[i, w] = next_k(v)
        for ij in range(8):
            correct_ref[ij] = zero

        def step(_, rho_now):
            for ij in range(8):
                correct_ref[ij] = correct_ref[ij] + direct_ref[ij // 2, mine * 2 + ij % 2]
            rho_next = 1.0 / (2.0 * sigma - rho_now)
            along = jnp.broadcast_to(rho_next * rho_now, (8, 128))
            across = jnp.broadcast_to(2.0 * rho_next / half, (8, 128))

            def advance(i, w, v, image):
                r = residual_ref[i, w] - image
                residual_ref[i, w] = r
                v = along * v + across * r
                direct_ref[i, w] = v
                turned_ref[i, w] = next_k(v)

            apply(advance)
            return rho_next

        lax.fori_loop(0, DEGREE, step, 1.0 / sigma)
        crosses = [zero] * 4
        squares = [zero] * 4
        for i, w in cells:
            s = start_ref[i, w]
            change = s - residual_ref[i, w]
            crosses[i] = crosses[i] + s * change
            squares[i] = squares[i] + change * change
        along = over_all((crosses[0] + crosses[1]) + (crosses[2] + crosses[3]))
        length = over_all((squares[0] + squares[1]) + (squares[2] + squares[3]))
        omega = jnp.broadcast_to(along / length, (8, 128))
        squares = [zero] * 4
        for i, w in cells:
            s = start_ref[i, w]
            r = s - omega * (s - residual_ref[i, w])
            residual_ref[i, w] = r
            squares[i] = squares[i] + r * r
        for ij in range(8):
            if sweep == 0:
                solution_ref[ij] = omega * correct_ref[ij]
            else:
                solution_ref[ij] = solution_ref[ij] + omega * correct_ref[ij]
        total = over_all((squares[0] + squares[1]) + (squares[2] + squares[3]))
        rms = jnp.broadcast_to(jnp.sqrt(total / 65536.0), (8, 128))
        if sweep == 0:
            history = rms
        else:
            history = jnp.where(lane == sweep, rms, history)

    for y, tile in enumerate(exchange_rows([solution_ref[ij] for ij in range(8)])):
        out_ref[y * 8 : y * 8 + 8, 0:128] = exchange_lanes(tile)
        out_ref[y * 8 : y * 8 + 8, 128:256] = history


def field(*lead):
    return pltpu.VMEM((*lead, 8, 128), jnp.float32)


def solve(parts):
    whole = field(4, 16)
    return pl.pallas_call(
        solve_kernel,
        out_shape=jax.ShapeDtypeStruct((64, 256), jnp.float32),
        scratch_shapes=[
            whole, whole, whole, whole, field(4, 4, 16), field(8), field(8),
        ],
        compiler_params=SMALL,
        name="solve",
    )(parts)


def in_hbm(array):
    return pltpu.with_memory_space_constraint(array, pltpu.HBM)


def on_device(right_side, links, coefs, reaction):
    message, order = pl.pallas_call(
        pack_kernel,
        out_shape=(jax.ShapeDtypeStruct((64, 384), jnp.float32), jax.ShapeDtypeStruct((128, 128), jnp.float32)),
        in_specs=[pl.BlockSpec(memory_space=pltpu.HBM)] * 4,
        scratch_shapes=[
            pltpu.VMEM((64, 128), jnp.float32), pltpu.VMEM((8, 128), jnp.int32),
            pltpu.VMEM((1, 128), jnp.float32), pltpu.VMEM((1, 128), jnp.float32), pltpu.SemaphoreType.DMA((4,)),
        ],
        compiler_params=SMALL,
        name="pack",
    )(*(in_hbm(a) for a in (right_side, links, coefs.reshape(1, 128), reaction.reshape(1, 128))))
    received = lax.all_to_all(message, ("grp", "z"), 0, 0, tiled=True)
    spread = pl.pallas_call(
        spread_kernel,
        out_shape=jax.ShapeDtypeStruct((4, 3, 8, 8, 128), jnp.float32),
        compiler_params=SMALL,
        name="spread",
    )(received)
    parts = lax.all_gather(lax.all_to_all(spread, "x", 0, 0, tiled=True), "core", axis=0)
    answer = solve(parts)
    answer = lax.all_to_all(answer, ("grp", "z"), 0, 0, tiled=True)
    return pl.pallas_call(
        unpack_kernel,
        out_shape=(jax.ShapeDtypeStruct((64, 128), jnp.float32), jax.ShapeDtypeStruct((SWEEPS, 64), jnp.float32)),
        compiler_params=SMALL,
        name="unpack",
    )(answer, order)


def solution(mesh):
    finer = Mesh(mesh.devices.reshape(8, 8, 4, 2), ("grp", "z", "x", "core"))
    blocks = ("grp", "z", "x", "core")
    return jax.shard_map(
        on_device,
        mesh=finer,
        in_specs=(P(None, blocks), P(None, blocks), P(blocks), P(blocks)),
        out_specs=(P(None, blocks), P()),
        check_vma=False,
    )
```

```python
import jax
import jax.numpy as jnp
from jax import lax
from jax.experimental import pallas as pl
from jax.experimental.pallas import tpu as pltpu
from jax.sharding import Mesh
from jax.sharding import PartitionSpec as P

SWEEPS = 2
DEGREE = 4
HIGHEST = lax.Precision.HIGHEST
SMALL = pltpu.CompilerParams(vmem_limit_bytes=16 * 1024 * 1024)


def dot(a, b, dims=((1,), (0,))):
    return lax.dot_general(a, b, (dims, ((), ())), precision=HIGHEST, preferred_element_type=jnp.float32)


def orders_of(links_ref):
    row = lax.broadcasted_iota(jnp.int32, (128, 128), 0)
    lane = lax.broadcasted_iota(jnp.int32, (128, 128), 1)
    regroup = (row == (lane % 8) * 16 + lane // 8).astype(jnp.bfloat16)
    onehot = (row == (links_ref[0:1, :] & 127)).astype(jnp.bfloat16)
    order = jnp.dot(onehot, regroup, preferred_element_type=jnp.float32)
    return regroup.astype(jnp.float32), order


def pack_kernel(right_hbm, links_hbm, coefs_hbm, reaction_hbm, message_ref, order_ref, right_ref, links_ref, coefs_ref, reaction_ref, semaphores):
    copies = [
        pltpu.make_async_copy(source, target, semaphores.at[n])
        for n, (source, target) in enumerate(
            [(links_hbm, links_ref), (right_hbm, right_ref), (coefs_hbm, coefs_ref), (reaction_hbm, reaction_ref)]
        )
    ]
    for copy in copies:
        copy.start()
    copies[0].wait()
    regroup, order = orders_of(links_ref)
    order_ref[...] = order
    for copy in copies[1:]:
        copy.wait()
    message_ref[:, 0:128] = dot(right_ref[...], order)
    coefs = dot(jnp.broadcast_to(coefs_ref[...], (8, 128)), regroup)
    reaction = dot(jnp.broadcast_to(reaction_ref[...], (8, 128)), order)
    for block in range(8):
        message_ref[block * 8 : block * 8 + 8, 128:256] = coefs
        message_ref[block * 8 : block * 8 + 8, 256:384] = reaction


def unpack_kernel(message_ref, order_ref, solution_ref, history_ref):
    solution_ref[...] = dot(message_ref[:, 0:128], order_ref[...], ((1,), (1,)))
    history_ref[...] = jnp.transpose(message_ref[:, 128:256])[0:SWEEPS, :]


def exchange_lanes(tile):
    row = lax.broadcasted_iota(jnp.int32, (8, 128), 0)
    lane = lax.broadcasted_iota(jnp.int32, (8, 128), 1)
    for bit in (1, 2, 4):
        from_below = pltpu.roll(pltpu.roll(tile, 8 - bit, 0), bit, 1)
        from_above = pltpu.roll(pltpu.roll(tile, bit, 0), 128 - bit, 1)
        lane_bit = (lane & bit) != 0
        same = ((row & bit) != 0) == lane_bit
        tile = jnp.where(same, tile, jnp.where(lane_bit, from_below, from_above))
    return tile


def exchange_rows(tiles):
    row = lax.broadcasted_iota(jnp.int32, (8, 128), 0)
    tiles = list(tiles)
    for bit in (1, 2, 4):
        upper = (row & bit) != 0
        for a in range(8):
            if not a & bit:
                b = a | bit
                first, second = tiles[a], tiles[b]
                tiles[a] = jnp.where(upper, pltpu.roll(second, bit, 0), first)
                tiles[b] = jnp.where(upper, second, pltpu.roll(first, 8 - bit, 0))
    return tiles


def spread_kernel(message_ref, out_ref):
    for kind in range(3):
        tiles = [
            exchange_lanes(message_ref[y * 8 : y * 8 + 8, kind * 128 : kind * 128 + 128]) for y in range(8)
        ]
        for ij, tile in enumerate(exchange_rows(tiles)):
            for x in range(4):
                out_ref[x, kind, ij] = tile


def solve_kernel(
    parts_ref, out_ref, direct_ref, turned_ref, residual_ref, start_ref, coef_ref,
    correct_ref,
):
    lane = lax.broadcasted_iota(jnp.int32, (8, 128), 1)
    last_z = (lane & 7) == 7
    first_z = (lane & 7) == 0
    mine = lax.axis_index("x") * 2 + lax.axis_index("core")

    def next_z(v):
        return jnp.where(last_z, pltpu.roll(v, 7, 1), pltpu.roll(v, 127, 1))

    def prev_z(v):
        return jnp.where(first_z, pltpu.roll(v, 121, 1), pltpu.roll(v, 1, 1))

    def next_k(v):
        return pltpu.roll(v, 120, 1)

    def prev_k(v):
        return pltpu.roll(v, 8, 1)

    cells = [(i, w) for w in range(16) for i in range(4)]

    def given(kind, i, w):
        return parts_ref[w // 2 % 2, w // 4, kind, i * 2 + w % 2]

    def next_i(vs):
        return [vs[1], vs[2], vs[3], pltpu.roll(vs[0], 7, 0)]

    def prev_i(vs):
        return [pltpu.roll(vs[3], 1, 0), vs[0], vs[1], vs[2]]

    def mul(a, b):
        return [p * q for p, q in zip(a, b)]

    def add(a, b):
        return [p + q for p, q in zip(a, b)]

    def sub(a, b):
        return [p - q for p, q in zip(a, b)]

    below = [[given(1, i, w) * (1.0 / 48.0) for i in range(4)] for w in range(16)]
    both = [add(vs, prev_i(vs)) for vs in below]
    for w in range(16):
        if w:
            below_pair, both_pair = add(below[w], below[w - 1]), add(both[w], both[w - 1])
        else:
            below_pair = add(below[0], [prev_z(v) for v in below[15]])
            both_pair = add(both[0], [prev_z(v) for v in both[15]])
        for i in range(4):
            v = given(0, i, w)
            direct_ref[i, w] = v
            turned_ref[i, w] = next_k(v)
            coef_ref[0, i, w] = below[w][i]
            coef_ref[1, i, w] = below[w][i] * 3.0
            coef_ref[2, i, w] = both[w][i] * 5.0
            coef_ref[3, i, w] = both[w][i] * 2.0
            coef_ref[4, i, w] = below_pair[i] * 2.0
            coef_ref[5, i, w] = both_pair[i] * 10.0

    def apply(visit):
        def load(w):
            here = [direct_ref[i, w] for i in range(4)]
            turned = [turned_ref[i, w] for i in range(4)]
            return add(here, turned), sub(turned, here)

        def coef(n, w):
            return [coef_ref[n, i, w] for i in range(4)]

        def couple(center, side, vs):
            return add(add(mul(center, vs), mul(side, next_i(vs))), prev_i(mul(side, vs)))

        def column(w, here, there):
            total, differ = add(here[0], there[0]), sub(there[0], here[0])
            flux = mul(coef(1, w), sub(next_i(total), total))
            total = sub(prev_i(flux), flux)
            differ = couple(coef(2, w), coef(0, w), differ)
            return sub(total, differ), add(total, differ), mul(coef(3, w), sub(there[1], here[1]))

        def finish(w, here, now, before):
            totals = add(now[0], before[1])
            differs = add(couple(coef(5, w), coef(4, w), here[1]), sub(now[2], before[2]))
            for i in range(4):
                v = direct_ref[i, w]
                visit(i, w, v, ((totals[i] - differs[i]) + given(2, i, w) * v) + prev_k(totals[i] + differs[i]))

        first, last = load(0), load(15)
        wrapped = [next_z(direct_ref[i, 0]) for i in range(4)]
        turned = [next_k(v) for v in wrapped]
        kept = column(15, last, (add(wrapped, turned), sub(turned, wrapped)))
        before = [[prev_z(v) for v in vs] for vs in kept]
        here = first
        for w in range(15):
            there = load(w + 1) if w < 14 else last
            now = column(w, here, there)
            finish(w, here, now, before)
            here, before = there, now
        finish(15, last, kept, before)

    def over_all(v):
        return jnp.sum(jnp.sum(v, axis=1, keepdims=True), axis=0, keepdims=True)

    zero = jnp.zeros((8, 128), jnp.float32)

    crosses = [zero] * 4
    squares = [zero] * 4

    def measure(i, w, v, image):
        crosses[i] = crosses[i] + v * image
        squares[i] = squares[i] + image * image

    apply(measure)
    cross = over_all((crosses[0] + crosses[1]) + (crosses[2] + crosses[3]))
    square = over_all((squares[0] + squares[1]) + (squares[2] + squares[3]))
    theta = square / cross
    upper = 1.5 * theta
    lower = upper / 10.0
    center = (upper + lower) / 2.0
    half = (upper - lower) / 2.0
    sigma = center / half
    per_center = 1.0 / center

    start_of = lambda i, w: given(0, i, w)
    scale = jnp.broadcast_to(per_center, (8, 128))
    for i, w in cells:
        v = given(0, i, w) * scale
        direct_ref[i, w] = v
        turned_ref[i, w] = next_k(v)

    for sweep in range(SWEEPS):
        for ij in range(8):
            correct_ref[ij] = zero
        for i, w in cells:
            residual_ref[i, w] = start_of(i, w)

        def correct():
            for ij in range(8):
                correct_ref[ij] = correct_ref[ij] + direct_ref[ij // 2, mine * 2 + ij % 2]

        def step(_, rho_now):
            correct()
            rho_next = 1.0 / (2.0 * sigma - rho_now)
            along = jnp.broadcast_to(rho_next * rho_now, (8, 128))
            across = jnp.broadcast_to(2.0 * rho_next / half, (8, 128))

            def advance(i, w, v, image):
                r = residual_ref[i, w] - image
                residual_ref[i, w] = r
                v = along * v + across * r
                direct_ref[i, w] = v
                turned_ref[i, w] = next_k(v)

            apply(advance)
            return rho_next

        lax.fori_loop(0, DEGREE - 1, step, 1.0 / sigma)
        correct()
        crosses = [zero] * 4
        squares = [zero] * 4

        def finish_sweep(i, w, v, image):
            r = residual_ref[i, w] - image
            residual_ref[i, w] = r
            s = start_of(i, w)
            change = s - r
            crosses[i] = crosses[i] + s * change
            squares[i] = squares[i] + change * change

        apply(finish_sweep)
        along = over_all((crosses[0] + crosses[1]) + (crosses[2] + crosses[3]))
        length = over_all((squares[0] + squares[1]) + (squares[2] + squares[3]))
        omega = jnp.broadcast_to(along / length, (8, 128))
        squares = [zero] * 4
        for i, w in cells:
            s = start_of(i, w)
            r = s - omega * (s - residual_ref[i, w])
            squares[i] = squares[i] + r * r
            if sweep < SWEEPS - 1:
                start_ref[i, w] = r
                v = r * scale
                direct_ref[i, w] = v
                turned_ref[i, w] = next_k(v)
        start_of = lambda i, w: start_ref[i, w]
        total = over_all((squares[0] + squares[1]) + (squares[2] + squares[3]))
        rms = jnp.broadcast_to(jnp.sqrt(total / 65536.0), (8, 128))
        if sweep == 0:
            history = rms
            answer = [omega * correct_ref[ij] for ij in range(8)]
        else:
            history = jnp.where(lane == sweep, rms, history)
            answer = [a + omega * correct_ref[ij] for ij, a in enumerate(answer)]

    for y, tile in enumerate(exchange_rows(answer)):
        out_ref[y * 8 : y * 8 + 8, 0:128] = exchange_lanes(tile)
        out_ref[y * 8 : y * 8 + 8, 128:256] = history


def field(*lead):
    return pltpu.VMEM((*lead, 8, 128), jnp.float32)


def solve(parts):
    whole = field(4, 16)
    return pl.pallas_call(
        solve_kernel,
        out_shape=jax.ShapeDtypeStruct((64, 256), jnp.float32),
        scratch_shapes=[
            whole, whole, whole, whole, field(6, 4, 16), field(8),
        ],
        compiler_params=SMALL,
        name="solve",
    )(parts)


def in_hbm(array):
    return pltpu.with_memory_space_constraint(array, pltpu.HBM)


def on_device(right_side, links, coefs, reaction):
    message, order = pl.pallas_call(
        pack_kernel,
        out_shape=(jax.ShapeDtypeStruct((64, 384), jnp.float32), jax.ShapeDtypeStruct((128, 128), jnp.float32)),
        in_specs=[pl.BlockSpec(memory_space=pltpu.HBM)] * 4,
        scratch_shapes=[
            pltpu.VMEM((64, 128), jnp.float32), pltpu.VMEM((8, 128), jnp.int32),
            pltpu.VMEM((1, 128), jnp.float32), pltpu.VMEM((1, 128), jnp.float32), pltpu.SemaphoreType.DMA((4,)),
        ],
        compiler_params=SMALL,
        name="pack",
    )(*(in_hbm(a) for a in (right_side, links, coefs.reshape(1, 128), reaction.reshape(1, 128))))
    received = lax.all_to_all(message, ("grp", "z"), 0, 0, tiled=True)
    spread = pl.pallas_call(
        spread_kernel,
        out_shape=jax.ShapeDtypeStruct((4, 3, 8, 8, 128), jnp.float32),
        compiler_params=SMALL,
        name="spread",
    )(received)
    parts = lax.all_gather(lax.all_to_all(spread, "x", 0, 0, tiled=True), "core", axis=0)
    answer = solve(parts)
    answer = lax.all_to_all(answer, ("grp", "z"), 0, 0, tiled=True)
    return pl.pallas_call(
        unpack_kernel,
        out_shape=(jax.ShapeDtypeStruct((64, 128), jnp.float32), jax.ShapeDtypeStruct((SWEEPS, 64), jnp.float32)),
        compiler_params=SMALL,
        name="unpack",
    )(answer, order)


def solution(mesh):
    finer = Mesh(mesh.devices.reshape(8, 8, 4, 2), ("grp", "z", "x", "core"))
    blocks = ("grp", "z", "x", "core")
    return jax.shard_map(
        on_device,
        mesh=finer,
        in_specs=(P(None, blocks), P(None, blocks), P(blocks), P(blocks)),
        out_specs=(P(None, blocks), P()),
        check_vma=False,
    )
```

```python
import jax
import jax.numpy as jnp
from jax import lax
from jax.experimental import pallas as pl
from jax.experimental.pallas import tpu as pltpu
from jax.sharding import Mesh
from jax.sharding import PartitionSpec as P

SWEEPS = 2
DEGREE = 4
EARLY = 5
LATE = (13, 14, 15)
HIGHEST = lax.Precision.HIGHEST
SMALL = pltpu.CompilerParams(vmem_limit_bytes=16 * 1024 * 1024)


def dot(a, b, dims=((1,), (0,))):
    return lax.dot_general(a, b, (dims, ((), ())), precision=HIGHEST, preferred_element_type=jnp.float32)


def orders_of(links_ref):
    row = lax.broadcasted_iota(jnp.int32, (128, 128), 0)
    lane = lax.broadcasted_iota(jnp.int32, (128, 128), 1)
    regroup = (row == (lane % 8) * 16 + lane // 8).astype(jnp.bfloat16)
    onehot = (row == (links_ref[0:1, :] & 127)).astype(jnp.bfloat16)
    order = jnp.dot(onehot, regroup, preferred_element_type=jnp.float32)
    return regroup.astype(jnp.float32), order


def pack_kernel(right_hbm, links_hbm, coefs_hbm, reaction_hbm, message_ref, order_ref, right_ref, links_ref, coefs_ref, reaction_ref, semaphores):
    copies = [
        pltpu.make_async_copy(source, target, semaphores.at[n])
        for n, (source, target) in enumerate(
            [(links_hbm, links_ref), (right_hbm, right_ref), (coefs_hbm, coefs_ref), (reaction_hbm, reaction_ref)]
        )
    ]
    for copy in copies:
        copy.start()
    copies[0].wait()
    regroup, order = orders_of(links_ref)
    order_ref[...] = order
    for copy in copies[1:]:
        copy.wait()
    message_ref[:, 0:128] = dot(right_ref[...], order)
    coefs = dot(jnp.broadcast_to(coefs_ref[...], (8, 128)), regroup)
    reaction = dot(jnp.broadcast_to(reaction_ref[...], (8, 128)), order)
    for block in range(8):
        message_ref[block * 8 : block * 8 + 8, 128:256] = coefs
        message_ref[block * 8 : block * 8 + 8, 256:384] = reaction


def unpack_kernel(message_ref, order_ref, solution_ref, history_ref):
    solution_ref[...] = dot(message_ref[:, 0:128], order_ref[...], ((1,), (1,)))
    history_ref[...] = jnp.transpose(message_ref[:, 128:256])[0:SWEEPS, :]


def exchange_lanes(tile):
    row = lax.broadcasted_iota(jnp.int32, (8, 128), 0)
    lane = lax.broadcasted_iota(jnp.int32, (8, 128), 1)
    for bit in (1, 2, 4):
        from_below = pltpu.roll(pltpu.roll(tile, 8 - bit, 0), bit, 1)
        from_above = pltpu.roll(pltpu.roll(tile, bit, 0), 128 - bit, 1)
        lane_bit = (lane & bit) != 0
        same = ((row & bit) != 0) == lane_bit
        tile = jnp.where(same, tile, jnp.where(lane_bit, from_below, from_above))
    return tile


def exchange_rows(tiles):
    row = lax.broadcasted_iota(jnp.int32, (8, 128), 0)
    tiles = list(tiles)
    for bit in (1, 2, 4):
        upper = (row & bit) != 0
        for a in range(8):
            if not a & bit:
                b = a | bit
                first, second = tiles[a], tiles[b]
                tiles[a] = jnp.where(upper, pltpu.roll(second, bit, 0), first)
                tiles[b] = jnp.where(upper, second, pltpu.roll(first, 8 - bit, 0))
    return tiles


def spread_kernel(message_ref, out_ref):
    for kind in range(3):
        tiles = [
            exchange_lanes(message_ref[y * 8 : y * 8 + 8, kind * 128 : kind * 128 + 128]) for y in range(8)
        ]
        for ij, tile in enumerate(exchange_rows(tiles)):
            for x in range(4):
                out_ref[x, kind, ij] = tile


def solve_kernel(
    parts_ref, out_ref, direct_ref, turned_ref, residual_ref, start_ref, coef_ref,
    correct_ref,
):
    lane = lax.broadcasted_iota(jnp.int32, (8, 128), 1)
    last_z = (lane & 7) == 7
    first_z = (lane & 7) == 0
    mine = lax.axis_index("x") * 2 + lax.axis_index("core")

    def next_z(v):
        return jnp.where(last_z, pltpu.roll(v, 7, 1), pltpu.roll(v, 127, 1))

    def prev_z(v):
        return jnp.where(first_z, pltpu.roll(v, 121, 1), pltpu.roll(v, 1, 1))

    def next_k(v):
        return pltpu.roll(v, 120, 1)

    def prev_k(v):
        return pltpu.roll(v, 8, 1)

    cells = [(i, w) for w in range(16) for i in range(4)]

    def given(kind, i, w):
        return parts_ref[w // 2 % 2, w // 4, kind, i * 2 + w % 2]

    def next_i(vs):
        return [vs[1], vs[2], vs[3], pltpu.roll(vs[0], 7, 0)]

    def prev_i(vs):
        return [pltpu.roll(vs[3], 1, 0), vs[0], vs[1], vs[2]]

    def mul(a, b):
        return [p * q for p, q in zip(a, b)]

    def add(a, b):
        return [p + q for p, q in zip(a, b)]

    def sub(a, b):
        return [p - q for p, q in zip(a, b)]

    below = [[given(1, i, w) * (1.0 / 48.0) for i in range(4)] for w in range(16)]
    both = [add(vs, prev_i(vs)) for vs in below]
    for w in range(16):
        if w:
            below_pair, both_pair = add(below[w], below[w - 1]), add(both[w], both[w - 1])
        else:
            below_pair = add(below[0], [prev_z(v) for v in below[15]])
            both_pair = add(both[0], [prev_z(v) for v in both[15]])
        for i in range(4):
            coef_ref[0, i, w] = below[w][i]
            coef_ref[1, i, w] = below[w][i] * 3.0
            coef_ref[2, i, w] = both[w][i] * 5.0
            coef_ref[3, i, w] = both[w][i] * 2.0
            coef_ref[4, i, w] = below_pair[i] * 2.0
            coef_ref[5, i, w] = both_pair[i] * 10.0

    def save(i, w, v):
        direct_ref[i, w] = v
        if w not in LATE:
            turned_ref[i, w] = next_k(v)

    def apply(visit, of=lambda i, w: direct_ref[i, w], turned_of=lambda i, w: turned_ref[i, w]):
        def load(w):
            here = [of(i, w) for i in range(4)]
            turned = [next_k(here[i]) if w in LATE else turned_of(i, w) for i in range(4)]
            return add(here, turned), sub(turned, here)

        def coef(n, w):
            return [coef_ref[n, i, w] for i in range(4)]

        def couple(center, side, vs):
            return add(add(mul(center, vs), mul(side, next_i(vs))), prev_i(mul(side, vs)))

        def column(w, here, there):
            total, differ = add(here[0], there[0]), sub(there[0], here[0])
            flux = mul(coef(1, w), sub(next_i(total), total))
            total = sub(prev_i(flux), flux)
            differ = couple(coef(2, w), coef(0, w), differ)
            return sub(total, differ), add(total, differ), mul(coef(3, w), sub(there[1], here[1]))

        def finish(w, here, now, before):
            totals = add(now[0], before[1])
            differs = add(couple(coef(5, w), coef(4, w), here[1]), sub(now[2], before[2]))
            for i in range(4):
                v = of(i, w)
                visit(i, w, v, ((totals[i] - differs[i]) + given(2, i, w) * v) + prev_k(totals[i] + differs[i]))

        wrapped = [next_z(of(i, 0)) for i in range(4)]
        turned = [next_k(v) for v in wrapped]
        nodes = [load(w) for w in range(16)] + [(add(wrapped, turned), sub(turned, wrapped))]
        made = {}
        for w in (*range(EARLY), 15, *range(EARLY, 15)):
            made[w] = column(w, nodes[w], nodes[w + 1])
            if w == 15:
                made[-1] = [[prev_z(v) for v in vs] for vs in made[15]]
                for early in range(EARLY):
                    finish(early, nodes[early], made[early], made[early - 1])
            elif w >= EARLY:
                finish(w, nodes[w], made[w], made[w - 1])
        finish(15, nodes[15], made[15], made[14])

    def over_all(v):
        return jnp.sum(jnp.sum(v, axis=1, keepdims=True), axis=0, keepdims=True)

    zero = jnp.zeros((8, 128), jnp.float32)

    crosses = [zero] * 4
    squares = [zero] * 4

    def measure(i, w, v, image):
        crosses[i] = crosses[i] + v * image
        squares[i] = squares[i] + image * image
        start_ref[i, w] = image

    apply(measure, lambda i, w: given(0, i, w), lambda i, w: next_k(given(0, i, w)))
    cross = over_all((crosses[0] + crosses[1]) + (crosses[2] + crosses[3]))
    square = over_all((squares[0] + squares[1]) + (squares[2] + squares[3]))
    theta = square / cross
    upper = 1.5 * theta
    lower = upper / 10.0
    center = (upper + lower) / 2.0
    half = (upper - lower) / 2.0
    sigma = center / half
    per_center = 1.0 / center

    def advanced(rho_now):
        rho_next = 1.0 / (2.0 * sigma - rho_now)
        return rho_next, jnp.broadcast_to(rho_next * rho_now, (8, 128)), jnp.broadcast_to(2.0 * rho_next / half, (8, 128))

    start_of = lambda i, w: given(0, i, w)
    scale = jnp.broadcast_to(per_center, (8, 128))
    rho_first, along, across = advanced(1.0 / sigma)
    for i, w in cells:
        s = start_of(i, w)
        r = s - start_ref[i, w] * scale
        residual_ref[i, w] = r
        save(i, w, along * (s * scale) + across * r)
    for ij in range(8):
        correct_ref[ij] = parts_ref[lax.axis_index("core"), lax.axis_index("x"), 0, ij] * scale

    for sweep in range(SWEEPS):
        if sweep:
            for ij in range(8):
                correct_ref[ij] = zero
            for i, w in cells:
                residual_ref[i, w] = start_of(i, w)

        def correct():
            for ij in range(8):
                correct_ref[ij] = correct_ref[ij] + direct_ref[ij // 2, mine * 2 + ij % 2]

        def step(_, rho_now):
            correct()
            rho_next, along, across = advanced(rho_now)

            def advance(i, w, v, image):
                r = residual_ref[i, w] - image
                residual_ref[i, w] = r
                save(i, w, along * v + across * r)

            apply(advance)
            return rho_next

        if sweep:
            lax.fori_loop(0, DEGREE - 1, step, 1.0 / sigma)
        else:
            lax.fori_loop(1, DEGREE - 1, step, rho_first)
        correct()
        crosses = [zero] * 4
        squares = [zero] * 4

        def finish_sweep(i, w, v, image):
            r = residual_ref[i, w] - image
            residual_ref[i, w] = r
            s = start_of(i, w)
            change = s - r
            crosses[i] = crosses[i] + s * change
            squares[i] = squares[i] + change * change

        apply(finish_sweep)
        along = over_all((crosses[0] + crosses[1]) + (crosses[2] + crosses[3]))
        length = over_all((squares[0] + squares[1]) + (squares[2] + squares[3]))
        omega = jnp.broadcast_to(along / length, (8, 128))
        squares = [zero] * 4
        for i, w in cells:
            s = start_of(i, w)
            r = s - omega * (s - residual_ref[i, w])
            squares[i] = squares[i] + r * r
            if sweep < SWEEPS - 1:
                start_ref[i, w] = r
                save(i, w, r * scale)
        start_of = lambda i, w: start_ref[i, w]
        total = over_all((squares[0] + squares[1]) + (squares[2] + squares[3]))
        rms = jnp.broadcast_to(jnp.sqrt(total / 65536.0), (8, 128))
        if sweep == 0:
            history = rms
            answer = [omega * correct_ref[ij] for ij in range(8)]
        else:
            history = jnp.where(lane == sweep, rms, history)
            answer = [a + omega * correct_ref[ij] for ij, a in enumerate(answer)]

    for y, tile in enumerate(exchange_rows(answer)):
        out_ref[y * 8 : y * 8 + 8, 0:128] = exchange_lanes(tile)
        out_ref[y * 8 : y * 8 + 8, 128:256] = history


def field(*lead):
    return pltpu.VMEM((*lead, 8, 128), jnp.float32)


def solve(parts):
    whole = field(4, 16)
    return pl.pallas_call(
        solve_kernel,
        out_shape=jax.ShapeDtypeStruct((64, 256), jnp.float32),
        scratch_shapes=[
            whole, whole, whole, whole, field(6, 4, 16), field(8),
        ],
        compiler_params=SMALL,
        name="solve",
    )(parts)


def in_hbm(array):
    return pltpu.with_memory_space_constraint(array, pltpu.HBM)


def on_device(right_side, links, coefs, reaction):
    message, order = pl.pallas_call(
        pack_kernel,
        out_shape=(jax.ShapeDtypeStruct((64, 384), jnp.float32), jax.ShapeDtypeStruct((128, 128), jnp.float32)),
        in_specs=[pl.BlockSpec(memory_space=pltpu.HBM)] * 4,
        scratch_shapes=[
            pltpu.VMEM((64, 128), jnp.float32), pltpu.VMEM((8, 128), jnp.int32),
            pltpu.VMEM((1, 128), jnp.float32), pltpu.VMEM((1, 128), jnp.float32), pltpu.SemaphoreType.DMA((4,)),
        ],
        compiler_params=SMALL,
        name="pack",
    )(*(in_hbm(a) for a in (right_side, links, coefs.reshape(1, 128), reaction.reshape(1, 128))))
    received = lax.all_to_all(message, ("grp", "z"), 0, 0, tiled=True)
    spread = pl.pallas_call(
        spread_kernel,
        out_shape=jax.ShapeDtypeStruct((4, 3, 8, 8, 128), jnp.float32),
        compiler_params=SMALL,
        name="spread",
    )(received)
    parts = lax.all_gather(lax.all_to_all(spread, "x", 0, 0, tiled=True), "core", axis=0)
    answer = solve(parts)
    answer = lax.all_to_all(answer, ("grp", "z"), 0, 0, tiled=True)
    return pl.pallas_call(
        unpack_kernel,
        out_shape=(jax.ShapeDtypeStruct((64, 128), jnp.float32), jax.ShapeDtypeStruct((SWEEPS, 64), jnp.float32)),
        compiler_params=SMALL,
        name="unpack",
    )(answer, order)


def solution(mesh):
    finer = Mesh(mesh.devices.reshape(8, 8, 4, 2), ("grp", "z", "x", "core"))
    blocks = ("grp", "z", "x", "core")
    return jax.shard_map(
        on_device,
        mesh=finer,
        in_specs=(P(None, blocks), P(None, blocks), P(blocks), P(blocks)),
        out_specs=(P(None, blocks), P()),
        check_vma=False,
    )
```

```python
import jax
import jax.numpy as jnp
from jax import lax
from jax.experimental import pallas as pl
from jax.experimental.pallas import tpu as pltpu
from jax.sharding import Mesh
from jax.sharding import PartitionSpec as P

SWEEPS = 2
DEGREE = 4
CENTER = (1.5 + 0.15) / 2.0
HALF = (1.5 - 0.15) / 2.0
RHOS = [HALF / CENTER]
for _ in range(DEGREE - 1):
    RHOS.append(1.0 / (2.0 * CENTER / HALF - RHOS[-1]))
EARLY = 5
LATE = (13, 14, 15)
SMALL = pltpu.CompilerParams(vmem_limit_bytes=16 * 1024 * 1024)


def pick(values, onehot, dims=((1,), (0,))):
    rows = values.shape[0]
    high = values.astype(jnp.bfloat16)
    rest = values - high.astype(jnp.float32)
    middle = rest.astype(jnp.bfloat16)
    low = (rest - middle.astype(jnp.float32)).astype(jnp.bfloat16)
    parts = [
        lax.dot_general(part, onehot, (dims, ((), ())), preferred_element_type=jnp.float32)
        for part in (high, middle, low)
    ]
    return (parts[2] + parts[1]) + parts[0]


def orders_of(links_ref):
    row = lax.broadcasted_iota(jnp.int32, (128, 128), 0)
    lane = lax.broadcasted_iota(jnp.int32, (128, 128), 1)
    regroup = (row == (lane % 8) * 16 + lane // 8).astype(jnp.bfloat16)
    onehot = (row == (links_ref[0:1, :] & 127)).astype(jnp.bfloat16)
    order = jnp.dot(onehot, regroup, preferred_element_type=jnp.float32)
    return regroup, order.astype(jnp.bfloat16)


def pack_kernel(right_hbm, links_hbm, coefs_hbm, reaction_hbm, message_ref, order_ref, right_ref, links_ref, coefs_ref, reaction_ref, semaphores):
    copies = [
        pltpu.make_async_copy(source, target, semaphores.at[n])
        for n, (source, target) in enumerate(
            [(links_hbm, links_ref), (right_hbm, right_ref), (coefs_hbm, coefs_ref), (reaction_hbm, reaction_ref)]
        )
    ]
    for copy in copies:
        copy.start()
    copies[0].wait()
    regroup, order = orders_of(links_ref)
    order_ref[...] = order
    for copy in copies[1:]:
        copy.wait()
    message_ref[:, 0:128] = pick(right_ref[...], order)
    coefs = pick(jnp.broadcast_to(coefs_ref[...], (8, 128)), regroup)
    reaction = pick(jnp.broadcast_to(reaction_ref[...], (8, 128)), order)
    for block in range(8):
        message_ref[block * 8 : block * 8 + 8, 128:256] = coefs
        message_ref[block * 8 : block * 8 + 8, 256:384] = reaction


def unpack_kernel(message_ref, order_ref, solution_ref, history_ref):
    solution_ref[...] = pick(message_ref[:, 0:128], order_ref[...], ((1,), (1,)))
    history_ref[...] = jnp.transpose(message_ref[:, 128:256])[0:SWEEPS, :]


def exchange_lanes(tile):
    row = lax.broadcasted_iota(jnp.int32, (8, 128), 0)
    lane = lax.broadcasted_iota(jnp.int32, (8, 128), 1)
    for bit in (1, 2, 4):
        from_below = pltpu.roll(pltpu.roll(tile, 8 - bit, 0), bit, 1)
        from_above = pltpu.roll(pltpu.roll(tile, bit, 0), 128 - bit, 1)
        lane_bit = (lane & bit) != 0
        same = ((row & bit) != 0) == lane_bit
        tile = jnp.where(same, tile, jnp.where(lane_bit, from_below, from_above))
    return tile


def exchange_rows(tiles):
    row = lax.broadcasted_iota(jnp.int32, (8, 128), 0)
    tiles = list(tiles)
    for bit in (1, 2, 4):
        upper = (row & bit) != 0
        for a in range(8):
            if not a & bit:
                b = a | bit
                first, second = tiles[a], tiles[b]
                tiles[a] = jnp.where(upper, pltpu.roll(second, bit, 0), first)
                tiles[b] = jnp.where(upper, second, pltpu.roll(first, 8 - bit, 0))
    return tiles


def spread_kernel(message_ref, out_ref):
    for kind in range(3):
        tiles = [
            exchange_lanes(message_ref[y * 8 : y * 8 + 8, kind * 128 : kind * 128 + 128]) for y in range(8)
        ]
        for ij, tile in enumerate(exchange_rows(tiles)):
            for x in range(4):
                out_ref[x, kind, ij] = tile


def solve_kernel(
    parts_ref, out_ref, direct_ref, turned_ref, residual_ref, start_ref, coef_ref,
    correct_ref,
):
    lane = lax.broadcasted_iota(jnp.int32, (8, 128), 1)
    last_z = (lane & 7) == 7
    first_z = (lane & 7) == 0
    mine = lax.axis_index("x") * 2 + lax.axis_index("core")

    def next_z(v):
        return jnp.where(last_z, pltpu.roll(v, 7, 1), pltpu.roll(v, 127, 1))

    def prev_z(v):
        return jnp.where(first_z, pltpu.roll(v, 121, 1), pltpu.roll(v, 1, 1))

    def next_k(v):
        return pltpu.roll(v, 120, 1)

    def prev_k(v):
        return pltpu.roll(v, 8, 1)

    cells = [(i, w) for w in range(16) for i in range(4)]

    def given(kind, i, w):
        return parts_ref[w // 2 % 2, w // 4, kind, i * 2 + w % 2]

    def next_i(vs):
        return [vs[1], vs[2], vs[3], pltpu.roll(vs[0], 7, 0)]

    def prev_i(vs):
        return [pltpu.roll(vs[3], 1, 0), vs[0], vs[1], vs[2]]

    def mul(a, b):
        return [p * q for p, q in zip(a, b)]

    def add(a, b):
        return [p + q for p, q in zip(a, b)]

    def sub(a, b):
        return [p - q for p, q in zip(a, b)]

    below = [[given(1, i, w) * (1.0 / 48.0) for i in range(4)] for w in range(16)]
    both = [add(vs, prev_i(vs)) for vs in below]
    for w in range(16):
        if w:
            below_pair, both_pair = add(below[w], below[w - 1]), add(both[w], both[w - 1])
        else:
            below_pair = add(below[0], [prev_z(v) for v in below[15]])
            both_pair = add(both[0], [prev_z(v) for v in both[15]])
        for i in range(4):
            coef_ref[0, i, w] = below[w][i]
            coef_ref[1, i, w] = below[w][i] * 3.0
            coef_ref[2, i, w] = both[w][i] * 5.0
            coef_ref[3, i, w] = both[w][i] * 2.0
            coef_ref[4, i, w] = below_pair[i] * 2.0
            coef_ref[5, i, w] = both_pair[i] * 10.0

    def save(i, w, v):
        direct_ref[i, w] = v
        if w not in LATE:
            turned_ref[i, w] = next_k(v)

    def apply(visit, of=lambda i, w: direct_ref[i, w], turned_of=lambda i, w: turned_ref[i, w]):
        def load(w):
            here = [of(i, w) for i in range(4)]
            turned = [next_k(here[i]) if w in LATE else turned_of(i, w) for i in range(4)]
            return add(here, turned), sub(turned, here)

        def coef(n, w):
            return [coef_ref[n, i, w] for i in range(4)]

        def couple(center, side, vs):
            return add(add(mul(center, vs), mul(side, next_i(vs))), prev_i(mul(side, vs)))

        def column(w, here, there):
            total, differ = add(here[0], there[0]), sub(there[0], here[0])
            flux = mul(coef(1, w), sub(next_i(total), total))
            total = sub(prev_i(flux), flux)
            differ = couple(coef(2, w), coef(0, w), differ)
            return sub(total, differ), add(total, differ), mul(coef(3, w), sub(there[1], here[1]))

        def finish(w, here, now, before):
            totals = add(now[0], before[1])
            differs = add(couple(coef(5, w), coef(4, w), here[1]), sub(now[2], before[2]))
            for i in range(4):
                v = of(i, w)
                visit(i, w, v, ((totals[i] - differs[i]) + given(2, i, w) * v) + prev_k(totals[i] + differs[i]))

        wrapped = [next_z(of(i, 0)) for i in range(4)]
        turned = [next_k(v) for v in wrapped]
        nodes = [load(w) for w in range(16)] + [(add(wrapped, turned), sub(turned, wrapped))]
        made = {}
        for w in (*range(EARLY), 15, *range(EARLY, 15)):
            made[w] = column(w, nodes[w], nodes[w + 1])
            if w == 15:
                made[-1] = [[prev_z(v) for v in vs] for vs in made[15]]
                for early in range(EARLY):
                    finish(early, nodes[early], made[early], made[early - 1])
            elif w >= EARLY:
                finish(w, nodes[w], made[w], made[w - 1])
        finish(15, nodes[15], made[15], made[14])

    def over_all(v):
        return jnp.sum(jnp.sum(v, axis=1, keepdims=True), axis=0, keepdims=True)

    zero = jnp.zeros((8, 128), jnp.float32)

    crosses = [zero] * 4
    squares = [zero] * 4

    def measure(i, w, v, image):
        crosses[i] = crosses[i] + v * image
        squares[i] = squares[i] + image * image
        start_ref[i, w] = image

    apply(measure, lambda i, w: given(0, i, w), lambda i, w: next_k(given(0, i, w)))
    cross = over_all((crosses[0] + crosses[1]) + (crosses[2] + crosses[3]))
    square = over_all((squares[0] + squares[1]) + (squares[2] + squares[3]))
    per_theta = cross / square

    def advanced(step):
        kept, added = RHOS[1] * RHOS[0], 2.0 * RHOS[1] / HALF
        if not isinstance(step, int) or step:
            for n in range(1, DEGREE - 1):
                kept = jnp.where(step == n, RHOS[n + 1] * RHOS[n], kept)
                added = jnp.where(step == n, 2.0 * RHOS[n + 1] / HALF, added)
        return kept, jnp.broadcast_to(added * per_theta, (8, 128))

    start_of = lambda i, w: given(0, i, w)
    scale = jnp.broadcast_to(per_theta * (1.0 / CENTER), (8, 128))
    along, across = advanced(0)
    for i, w in cells:
        s = start_of(i, w)
        r = s - start_ref[i, w] * scale
        residual_ref[i, w] = r
        save(i, w, along * (s * scale) + across * r)
    for ij in range(8):
        correct_ref[ij] = parts_ref[lax.axis_index("core"), lax.axis_index("x"), 0, ij] * scale

    for sweep in range(SWEEPS):
        if sweep:
            for ij in range(8):
                correct_ref[ij] = zero
            for i, w in cells:
                residual_ref[i, w] = start_of(i, w)

        def correct():
            for ij in range(8):
                correct_ref[ij] = correct_ref[ij] + direct_ref[ij // 2, mine * 2 + ij % 2]

        def step(number, carry):
            correct()
            along, across = advanced(number)

            def advance(i, w, v, image):
                r = residual_ref[i, w] - image
                residual_ref[i, w] = r
                save(i, w, along * v + across * r)

            apply(advance)
            return carry

        lax.fori_loop(0 if sweep else 1, DEGREE - 1, step, 0)
        correct()
        crosses = [zero] * 4
        squares = [zero] * 4

        def finish_sweep(i, w, v, image):
            r = residual_ref[i, w] - image
            residual_ref[i, w] = r
            s = start_of(i, w)
            change = s - r
            crosses[i] = crosses[i] + s * change
            squares[i] = squares[i] + change * change

        apply(finish_sweep)
        along = over_all((crosses[0] + crosses[1]) + (crosses[2] + crosses[3]))
        length = over_all((squares[0] + squares[1]) + (squares[2] + squares[3]))
        omega = jnp.broadcast_to(along / length, (8, 128))
        squares = [zero] * 4
        for i, w in cells:
            s = start_of(i, w)
            r = s - omega * (s - residual_ref[i, w])
            squares[i] = squares[i] + r * r
            if sweep < SWEEPS - 1:
                start_ref[i, w] = r
                save(i, w, r * scale)
        start_of = lambda i, w: start_ref[i, w]
        total = over_all((squares[0] + squares[1]) + (squares[2] + squares[3]))
        rms = jnp.broadcast_to(jnp.sqrt(total / 65536.0), (8, 128))
        if sweep == 0:
            history = rms
            answer = [omega * correct_ref[ij] for ij in range(8)]
        else:
            history = jnp.where(lane == sweep, rms, history)
            answer = [a + omega * correct_ref[ij] for ij, a in enumerate(answer)]

    for y, tile in enumerate(exchange_rows(answer)):
        out_ref[y * 8 : y * 8 + 8, 0:128] = exchange_lanes(tile)
        out_ref[y * 8 : y * 8 + 8, 128:256] = history


def field(*lead):
    return pltpu.VMEM((*lead, 8, 128), jnp.float32)


def solve(parts):
    whole = field(4, 16)
    return pl.pallas_call(
        solve_kernel,
        out_shape=jax.ShapeDtypeStruct((64, 256), jnp.float32),
        scratch_shapes=[
            whole, whole, whole, whole, field(6, 4, 16), field(8),
        ],
        compiler_params=SMALL,
        name="solve",
    )(parts)


def in_hbm(array):
    return pltpu.with_memory_space_constraint(array, pltpu.HBM)


def on_device(right_side, links, coefs, reaction):
    message, order = pl.pallas_call(
        pack_kernel,
        out_shape=(jax.ShapeDtypeStruct((64, 384), jnp.float32), jax.ShapeDtypeStruct((128, 128), jnp.bfloat16)),
        in_specs=[pl.BlockSpec(memory_space=pltpu.HBM)] * 4,
        scratch_shapes=[
            pltpu.VMEM((64, 128), jnp.float32), pltpu.VMEM((8, 128), jnp.int32),
            pltpu.VMEM((1, 128), jnp.float32), pltpu.VMEM((1, 128), jnp.float32), pltpu.SemaphoreType.DMA((4,)),
        ],
        compiler_params=SMALL,
        name="pack",
    )(*(in_hbm(a) for a in (right_side, links, coefs.reshape(1, 128), reaction.reshape(1, 128))))
    received = lax.all_to_all(message, ("grp", "z"), 0, 0, tiled=True)
    spread = pl.pallas_call(
        spread_kernel,
        out_shape=jax.ShapeDtypeStruct((4, 3, 8, 8, 128), jnp.float32),
        compiler_params=SMALL,
        name="spread",
    )(received)
    parts = lax.all_gather(lax.all_to_all(spread, "x", 0, 0, tiled=True), "core", axis=0)
    answer = solve(parts)
    answer = lax.all_to_all(answer, ("grp", "z"), 0, 0, tiled=True)
    return pl.pallas_call(
        unpack_kernel,
        out_shape=(jax.ShapeDtypeStruct((64, 128), jnp.float32), jax.ShapeDtypeStruct((SWEEPS, 64), jnp.float32)),
        compiler_params=SMALL,
        name="unpack",
    )(answer, order)


def solution(mesh):
    finer = Mesh(mesh.devices.reshape(8, 8, 4, 2), ("grp", "z", "x", "core"))
    blocks = ("grp", "z", "x", "core")
    return jax.shard_map(
        on_device,
        mesh=finer,
        in_specs=(P(None, blocks), P(None, blocks), P(blocks), P(blocks)),
        out_specs=(P(None, blocks), P()),
        check_vma=False,
    )
```

```python
import jax
import jax.numpy as jnp
from jax import lax
from jax.experimental import pallas as pl
from jax.experimental.pallas import tpu as pltpu
from jax.sharding import Mesh
from jax.sharding import PartitionSpec as P

SWEEPS = 2
DEGREE = 4
CENTER = (1.5 + 0.15) / 2.0
HALF = (1.5 - 0.15) / 2.0
RHOS = [HALF / CENTER]
for _ in range(DEGREE - 1):
    RHOS.append(1.0 / (2.0 * CENTER / HALF - RHOS[-1]))
EARLY = 5
LATE = (13, 14, 15)
SMALL = pltpu.CompilerParams(vmem_limit_bytes=16 * 1024 * 1024)


def pick(values, onehot, dims=((1,), (0,))):
    rows = values.shape[0]
    high = values.astype(jnp.bfloat16)
    rest = values - high.astype(jnp.float32)
    middle = rest.astype(jnp.bfloat16)
    low = (rest - middle.astype(jnp.float32)).astype(jnp.bfloat16)
    parts = [
        lax.dot_general(part, onehot, (dims, ((), ())), preferred_element_type=jnp.float32)
        for part in (high, middle, low)
    ]
    return (parts[2] + parts[1]) + parts[0]


def gather_lanes(values, lanes):
    return jnp.take_along_axis(values, jnp.broadcast_to(lanes[0:1], values.shape), axis=1, mode="promise_in_bounds")


def pack_kernel(right_hbm, links_hbm, coefs_hbm, reaction_hbm, message_ref, order_ref, right_ref, links_ref, coefs_ref, reaction_ref, semaphores):
    copies = [
        pltpu.make_async_copy(source, target, semaphores.at[n])
        for n, (source, target) in enumerate(
            [(links_hbm, links_ref), (right_hbm, right_ref), (coefs_hbm, coefs_ref), (reaction_hbm, reaction_ref)]
        )
    ]
    for copy in copies:
        copy.start()
    copies[0].wait()
    lane = lax.broadcasted_iota(jnp.int32, (8, 128), 1)
    element = (lane & 7) * 16 + (lane >> 3)
    slot = gather_lanes(jnp.broadcast_to(links_ref[0:1, :] & 127, (8, 128)), element)
    row = lax.broadcasted_iota(jnp.int32, (128, 128), 0)
    order_ref[...] = (row == slot[0:1]).astype(jnp.float32).astype(jnp.bfloat16)
    for copy in copies[1:]:
        copy.wait()
    message_ref[:, 0:128] = gather_lanes(right_ref[...], slot)
    coefs = gather_lanes(jnp.broadcast_to(coefs_ref[...], (8, 128)), element)
    reaction = gather_lanes(jnp.broadcast_to(reaction_ref[...], (8, 128)), slot)
    for block in range(8):
        message_ref[block * 8 : block * 8 + 8, 128:256] = coefs
        message_ref[block * 8 : block * 8 + 8, 256:384] = reaction


def unpack_kernel(message_ref, order_ref, solution_ref, history_ref):
    solution_ref[...] = pick(message_ref[:, 0:128], order_ref[...], ((1,), (1,)))
    history_ref[...] = jnp.transpose(message_ref[:, 128:256])[0:SWEEPS, :]


def exchange_lanes(tile):
    row = lax.broadcasted_iota(jnp.int32, (8, 128), 0)
    lane = lax.broadcasted_iota(jnp.int32, (8, 128), 1)
    for bit in (1, 2, 4):
        from_below = pltpu.roll(pltpu.roll(tile, 8 - bit, 0), bit, 1)
        from_above = pltpu.roll(pltpu.roll(tile, bit, 0), 128 - bit, 1)
        lane_bit = (lane & bit) != 0
        same = ((row & bit) != 0) == lane_bit
        tile = jnp.where(same, tile, jnp.where(lane_bit, from_below, from_above))
    return tile


def exchange_rows(tiles):
    row = lax.broadcasted_iota(jnp.int32, (8, 128), 0)
    tiles = list(tiles)
    for bit in (1, 2, 4):
        upper = (row & bit) != 0
        for a in range(8):
            if not a & bit:
                b = a | bit
                first, second = tiles[a], tiles[b]
                tiles[a] = jnp.where(upper, pltpu.roll(second, bit, 0), first)
                tiles[b] = jnp.where(upper, second, pltpu.roll(first, 8 - bit, 0))
    return tiles


def spread_kernel(message_ref, out_ref):
    for kind in range(3):
        tiles = [
            exchange_lanes(message_ref[y * 8 : y * 8 + 8, kind * 128 : kind * 128 + 128]) for y in range(8)
        ]
        for ij, tile in enumerate(exchange_rows(tiles)):
            for x in range(4):
                out_ref[x, kind, ij] = tile


def solve_kernel(
    parts_ref, out_ref, direct_ref, turned_ref, residual_ref, start_ref, coef_ref,
    correct_ref,
):
    lane = lax.broadcasted_iota(jnp.int32, (8, 128), 1)
    last_z = (lane & 7) == 7
    first_z = (lane & 7) == 0
    mine = lax.axis_index("x") * 2 + lax.axis_index("core")

    def next_z(v):
        return jnp.where(last_z, pltpu.roll(v, 7, 1), pltpu.roll(v, 127, 1))

    def prev_z(v):
        return jnp.where(first_z, pltpu.roll(v, 121, 1), pltpu.roll(v, 1, 1))

    def next_k(v):
        return pltpu.roll(v, 120, 1)

    def prev_k(v):
        return pltpu.roll(v, 8, 1)

    cells = [(i, w) for w in range(16) for i in range(4)]

    def given(kind, i, w):
        return parts_ref[w // 2 % 2, w // 4, kind, i * 2 + w % 2]

    def next_i(vs):
        return [vs[1], vs[2], vs[3], pltpu.roll(vs[0], 7, 0)]

    def prev_i(vs):
        return [pltpu.roll(vs[3], 1, 0), vs[0], vs[1], vs[2]]

    def mul(a, b):
        return [p * q for p, q in zip(a, b)]

    def add(a, b):
        return [p + q for p, q in zip(a, b)]

    def sub(a, b):
        return [p - q for p, q in zip(a, b)]

    below = [[given(1, i, w) * (1.0 / 48.0) for i in range(4)] for w in range(16)]
    both = [add(vs, prev_i(vs)) for vs in below]
    for w in range(16):
        if w:
            below_pair, both_pair = add(below[w], below[w - 1]), add(both[w], both[w - 1])
        else:
            below_pair = add(below[0], [prev_z(v) for v in below[15]])
            both_pair = add(both[0], [prev_z(v) for v in both[15]])
        for i in range(4):
            coef_ref[0, i, w] = below[w][i]
            coef_ref[1, i, w] = below[w][i] * 3.0
            coef_ref[2, i, w] = both[w][i] * 5.0
            coef_ref[3, i, w] = both[w][i] * 2.0
            coef_ref[4, i, w] = below_pair[i] * 2.0
            coef_ref[5, i, w] = both_pair[i] * 10.0

    def save(i, w, v):
        direct_ref[i, w] = v
        if w not in LATE:
            turned_ref[i, w] = next_k(v)

    def apply(visit, of=lambda i, w: direct_ref[i, w], turned_of=lambda i, w: turned_ref[i, w]):
        def load(w):
            here = [of(i, w) for i in range(4)]
            turned = [next_k(here[i]) if w in LATE else turned_of(i, w) for i in range(4)]
            return add(here, turned), sub(turned, here)

        def coef(n, w):
            return [coef_ref[n, i, w] for i in range(4)]

        def couple(center, side, vs):
            return add(add(mul(center, vs), mul(side, next_i(vs))), prev_i(mul(side, vs)))

        def column(w, here, there):
            total, differ = add(here[0], there[0]), sub(there[0], here[0])
            flux = mul(coef(1, w), sub(next_i(total), total))
            total = sub(prev_i(flux), flux)
            differ = couple(coef(2, w), coef(0, w), differ)
            return sub(total, differ), add(total, differ), mul(coef(3, w), sub(there[1], here[1]))

        def finish(w, here, now, before):
            totals = add(now[0], before[1])
            differs = add(couple(coef(5, w), coef(4, w), here[1]), sub(now[2], before[2]))
            for i in range(4):
                v = of(i, w)
                visit(i, w, v, ((totals[i] - differs[i]) + given(2, i, w) * v) + prev_k(totals[i] + differs[i]))

        wrapped = [next_z(of(i, 0)) for i in range(4)]
        turned = [next_k(v) for v in wrapped]
        nodes = [load(w) for w in range(16)] + [(add(wrapped, turned), sub(turned, wrapped))]
        made = {}
        for w in (*range(EARLY), 15, *range(EARLY, 15)):
            made[w] = column(w, nodes[w], nodes[w + 1])
            if w == 15:
                made[-1] = [[prev_z(v) for v in vs] for vs in made[15]]
                for early in range(EARLY):
                    finish(early, nodes[early], made[early], made[early - 1])
            elif w >= EARLY:
                finish(w, nodes[w], made[w], made[w - 1])
        finish(15, nodes[15], made[15], made[14])

    def over_all(v):
        return jnp.sum(jnp.sum(v, axis=1, keepdims=True), axis=0, keepdims=True)

    zero = jnp.zeros((8, 128), jnp.float32)

    crosses = [zero] * 4
    squares = [zero] * 4

    def measure(i, w, v, image):
        crosses[i] = crosses[i] + v * image
        squares[i] = squares[i] + image * image
        start_ref[i, w] = image

    apply(measure, lambda i, w: given(0, i, w), lambda i, w: next_k(given(0, i, w)))
    cross = over_all((crosses[0] + crosses[1]) + (crosses[2] + crosses[3]))
    square = over_all((squares[0] + squares[1]) + (squares[2] + squares[3]))
    per_theta = cross / square

    def advanced(step):
        kept, added = RHOS[1] * RHOS[0], 2.0 * RHOS[1] / HALF
        if not isinstance(step, int) or step:
            for n in range(1, DEGREE - 1):
                kept = jnp.where(step == n, RHOS[n + 1] * RHOS[n], kept)
                added = jnp.where(step == n, 2.0 * RHOS[n + 1] / HALF, added)
        return kept, jnp.broadcast_to(added * per_theta, (8, 128))

    start_of = lambda i, w: given(0, i, w)
    scale = jnp.broadcast_to(per_theta * (1.0 / CENTER), (8, 128))
    along, across = advanced(0)
    for i, w in cells:
        s = start_of(i, w)
        r = s - start_ref[i, w] * scale
        residual_ref[i, w] = r
        save(i, w, along * (s * scale) + across * r)
    for ij in range(8):
        correct_ref[ij] = parts_ref[lax.axis_index("core"), lax.axis_index("x"), 0, ij] * scale

    for sweep in range(SWEEPS):
        if sweep:
            for ij in range(8):
                correct_ref[ij] = zero
            for i, w in cells:
                residual_ref[i, w] = start_of(i, w)

        def correct():
            for ij in range(8):
                correct_ref[ij] = correct_ref[ij] + direct_ref[ij // 2, mine * 2 + ij % 2]

        def step(number, carry):
            correct()
            along, across = advanced(number)

            def advance(i, w, v, image):
                r = residual_ref[i, w] - image
                residual_ref[i, w] = r
                save(i, w, along * v + across * r)

            apply(advance)
            return carry

        lax.fori_loop(0 if sweep else 1, DEGREE - 1, step, 0)
        correct()
        crosses = [zero] * 4
        squares = [zero] * 4

        def finish_sweep(i, w, v, image):
            r = residual_ref[i, w] - image
            residual_ref[i, w] = r
            s = start_of(i, w)
            change = s - r
            crosses[i] = crosses[i] + s * change
            squares[i] = squares[i] + change * change

        apply(finish_sweep)
        along = over_all((crosses[0] + crosses[1]) + (crosses[2] + crosses[3]))
        length = over_all((squares[0] + squares[1]) + (squares[2] + squares[3]))
        omega = jnp.broadcast_to(along / length, (8, 128))
        squares = [zero] * 4
        for i, w in cells:
            s = start_of(i, w)
            r = s - omega * (s - residual_ref[i, w])
            squares[i] = squares[i] + r * r
            if sweep < SWEEPS - 1:
                start_ref[i, w] = r
                save(i, w, r * scale)
        start_of = lambda i, w: start_ref[i, w]
        total = over_all((squares[0] + squares[1]) + (squares[2] + squares[3]))
        rms = jnp.broadcast_to(jnp.sqrt(total / 65536.0), (8, 128))
        if sweep == 0:
            history = rms
            answer = [omega * correct_ref[ij] for ij in range(8)]
        else:
            history = jnp.where(lane == sweep, rms, history)
            answer = [a + omega * correct_ref[ij] for ij, a in enumerate(answer)]

    for y, tile in enumerate(exchange_rows(answer)):
        out_ref[y * 8 : y * 8 + 8, 0:128] = exchange_lanes(tile)
        out_ref[y * 8 : y * 8 + 8, 128:256] = history


def field(*lead):
    return pltpu.VMEM((*lead, 8, 128), jnp.float32)


def solve(parts):
    whole = field(4, 16)
    return pl.pallas_call(
        solve_kernel,
        out_shape=jax.ShapeDtypeStruct((64, 256), jnp.float32),
        scratch_shapes=[
            whole, whole, whole, whole, field(6, 4, 16), field(8),
        ],
        compiler_params=SMALL,
        name="solve",
    )(parts)


def in_hbm(array):
    return pltpu.with_memory_space_constraint(array, pltpu.HBM)


def on_device(right_side, links, coefs, reaction):
    message, order = pl.pallas_call(
        pack_kernel,
        out_shape=(jax.ShapeDtypeStruct((64, 384), jnp.float32), jax.ShapeDtypeStruct((128, 128), jnp.bfloat16)),
        in_specs=[pl.BlockSpec(memory_space=pltpu.HBM)] * 4,
        scratch_shapes=[
            pltpu.VMEM((64, 128), jnp.float32), pltpu.VMEM((8, 128), jnp.int32),
            pltpu.VMEM((1, 128), jnp.float32), pltpu.VMEM((1, 128), jnp.float32), pltpu.SemaphoreType.DMA((4,)),
        ],
        compiler_params=SMALL,
        name="pack",
    )(*(in_hbm(a) for a in (right_side, links, coefs.reshape(1, 128), reaction.reshape(1, 128))))
    received = lax.all_to_all(message, ("grp", "z"), 0, 0, tiled=True)
    spread = pl.pallas_call(
        spread_kernel,
        out_shape=jax.ShapeDtypeStruct((4, 3, 8, 8, 128), jnp.float32),
        compiler_params=SMALL,
        name="spread",
    )(received)
    parts = lax.all_gather(lax.all_to_all(spread, "x", 0, 0, tiled=True), "core", axis=0)
    answer = solve(parts)
    answer = lax.all_to_all(answer, ("grp", "z"), 0, 0, tiled=True)
    return pl.pallas_call(
        unpack_kernel,
        out_shape=(jax.ShapeDtypeStruct((64, 128), jnp.float32), jax.ShapeDtypeStruct((SWEEPS, 64), jnp.float32)),
        compiler_params=SMALL,
        name="unpack",
    )(answer, order)


def solution(mesh):
    finer = Mesh(mesh.devices.reshape(8, 8, 4, 2), ("grp", "z", "x", "core"))
    blocks = ("grp", "z", "x", "core")
    return jax.shard_map(
        on_device,
        mesh=finer,
        in_specs=(P(None, blocks), P(None, blocks), P(blocks), P(blocks)),
        out_specs=(P(None, blocks), P()),
        check_vma=False,
    )
```

```python
import jax
import jax.numpy as jnp
from jax import lax
from jax.experimental import pallas as pl
from jax.experimental.pallas import tpu as pltpu
from jax.sharding import Mesh
from jax.sharding import PartitionSpec as P

SWEEPS = 2
DEGREE = 4
CENTER = (1.5 + 0.15) / 2.0
HALF = (1.5 - 0.15) / 2.0
RHOS = [HALF / CENTER]
for _ in range(DEGREE - 1):
    RHOS.append(1.0 / (2.0 * CENTER / HALF - RHOS[-1]))
EARLY = 5
LATE = (13, 14, 15)
SMALL = pltpu.CompilerParams(vmem_limit_bytes=16 * 1024 * 1024)


def pick(values, onehot, dims=((1,), (0,))):
    rows = values.shape[0]
    high = values.astype(jnp.bfloat16)
    rest = values - high.astype(jnp.float32)
    middle = rest.astype(jnp.bfloat16)
    low = (rest - middle.astype(jnp.float32)).astype(jnp.bfloat16)
    parts = [
        lax.dot_general(part, onehot, (dims, ((), ())), preferred_element_type=jnp.float32)
        for part in (high, middle, low)
    ]
    return (parts[2] + parts[1]) + parts[0]


def gather_lanes(values, lanes):
    return jnp.take_along_axis(values, jnp.broadcast_to(lanes[0:1], values.shape), axis=1, mode="promise_in_bounds")


def pack_kernel(right_hbm, links_hbm, coefs_hbm, reaction_hbm, message_ref, order_ref, right_ref, links_ref, coefs_ref, reaction_ref, semaphores):
    copies = [
        pltpu.make_async_copy(source, target, semaphores.at[n])
        for n, (source, target) in enumerate(
            [(links_hbm, links_ref), (right_hbm, right_ref), (coefs_hbm, coefs_ref), (reaction_hbm, reaction_ref)]
        )
    ]
    for copy in copies:
        copy.start()
    copies[0].wait()
    lane = lax.broadcasted_iota(jnp.int32, (8, 128), 1)
    element = (lane & 7) * 16 + (lane >> 3)
    slot = gather_lanes(jnp.broadcast_to(links_ref[0:1, :] & 127, (8, 128)), element)
    row = lax.broadcasted_iota(jnp.int32, (128, 128), 0)
    order_ref[...] = (row == slot[0:1]).astype(jnp.float32).astype(jnp.bfloat16)
    for copy in copies[1:]:
        copy.wait()
    message_ref[:, 0, 0:128] = gather_lanes(right_ref[...], slot)
    coefs = gather_lanes(jnp.broadcast_to(coefs_ref[...], (8, 128)), element)
    reaction = gather_lanes(jnp.broadcast_to(reaction_ref[...], (8, 128)), slot)
    for block in range(8):
        message_ref[block * 8 : block * 8 + 8, 0, 128:256] = coefs
        message_ref[block * 8 : block * 8 + 8, 0, 256:384] = reaction


def unpack_kernel(message_ref, order_ref, solution_ref, history_ref):
    solution_ref[...] = pick(message_ref[:, 0:128], order_ref[...], ((1,), (1,)))
    history_ref[...] = jnp.transpose(message_ref[:, 128:256])[0:SWEEPS, :]


def exchange_lanes(tile):
    row = lax.broadcasted_iota(jnp.int32, (8, 128), 0)
    lane = lax.broadcasted_iota(jnp.int32, (8, 128), 1)
    for bit in (1, 2, 4):
        from_below = pltpu.roll(pltpu.roll(tile, 8 - bit, 0), bit, 1)
        from_above = pltpu.roll(pltpu.roll(tile, bit, 0), 128 - bit, 1)
        lane_bit = (lane & bit) != 0
        same = ((row & bit) != 0) == lane_bit
        tile = jnp.where(same, tile, jnp.where(lane_bit, from_below, from_above))
    return tile


def exchange_rows(tiles):
    row = lax.broadcasted_iota(jnp.int32, (8, 128), 0)
    tiles = list(tiles)
    for bit in (1, 2, 4):
        upper = (row & bit) != 0
        for a in range(8):
            if not a & bit:
                b = a | bit
                first, second = tiles[a], tiles[b]
                tiles[a] = jnp.where(upper, pltpu.roll(second, bit, 0), first)
                tiles[b] = jnp.where(upper, second, pltpu.roll(first, 8 - bit, 0))
    return tiles


def spread_kernel(message_ref, out_ref):
    for kind in range(3):
        tiles = [
            exchange_lanes(message_ref[y * 8 : y * 8 + 8, kind * 128 : kind * 128 + 128]) for y in range(8)
        ]
        for ij, tile in enumerate(exchange_rows(tiles)):
            for x in range(4):
                out_ref[x, kind, ij] = tile


def solve_kernel(
    parts_ref, out_ref, direct_ref, turned_ref, residual_ref, start_ref, coef_ref,
    correct_ref,
):
    lane = lax.broadcasted_iota(jnp.int32, (8, 128), 1)
    last_z = (lane & 7) == 7
    first_z = (lane & 7) == 0
    mine = lax.axis_index("x") * 2 + lax.axis_index("core")

    def next_z(v):
        return jnp.where(last_z, pltpu.roll(v, 7, 1), pltpu.roll(v, 127, 1))

    def prev_z(v):
        return jnp.where(first_z, pltpu.roll(v, 121, 1), pltpu.roll(v, 1, 1))

    def next_k(v):
        return pltpu.roll(v, 120, 1)

    def prev_k(v):
        return pltpu.roll(v, 8, 1)

    cells = [(i, w) for w in range(16) for i in range(4)]

    def given(kind, i, w):
        return parts_ref[w // 2 % 2, w // 4, kind, i * 2 + w % 2]

    def next_i(vs):
        return [vs[1], vs[2], vs[3], pltpu.roll(vs[0], 7, 0)]

    def prev_i(vs):
        return [pltpu.roll(vs[3], 1, 0), vs[0], vs[1], vs[2]]

    def mul(a, b):
        return [p * q for p, q in zip(a, b)]

    def add(a, b):
        return [p + q for p, q in zip(a, b)]

    def sub(a, b):
        return [p - q for p, q in zip(a, b)]

    below = [[given(1, i, w) * (1.0 / 48.0) for i in range(4)] for w in range(16)]
    both = [add(vs, prev_i(vs)) for vs in below]
    for w in range(16):
        if w:
            below_pair, both_pair = add(below[w], below[w - 1]), add(both[w], both[w - 1])
        else:
            below_pair = add(below[0], [prev_z(v) for v in below[15]])
            both_pair = add(both[0], [prev_z(v) for v in both[15]])
        for i in range(4):
            coef_ref[0, i, w] = below[w][i]
            coef_ref[1, i, w] = below[w][i] * 3.0
            coef_ref[2, i, w] = both[w][i] * 5.0
            coef_ref[3, i, w] = both[w][i] * 2.0
            coef_ref[4, i, w] = below_pair[i] * 2.0
            coef_ref[5, i, w] = both_pair[i] * 10.0

    def save(i, w, v):
        direct_ref[i, w] = v
        if w not in LATE:
            turned_ref[i, w] = next_k(v)

    def apply(visit, of=lambda i, w: direct_ref[i, w], turned_of=lambda i, w: turned_ref[i, w]):
        def load(w):
            here = [of(i, w) for i in range(4)]
            turned = [next_k(here[i]) if w in LATE else turned_of(i, w) for i in range(4)]
            return add(here, turned), sub(turned, here)

        def coef(n, w):
            return [coef_ref[n, i, w] for i in range(4)]

        def couple(center, side, vs):
            return add(add(mul(center, vs), mul(side, next_i(vs))), prev_i(mul(side, vs)))

        def column(w, here, there):
            total, differ = add(here[0], there[0]), sub(there[0], here[0])
            flux = mul(coef(1, w), sub(next_i(total), total))
            total = sub(prev_i(flux), flux)
            differ = couple(coef(2, w), coef(0, w), differ)
            return sub(total, differ), add(total, differ), mul(coef(3, w), sub(there[1], here[1]))

        def finish(w, here, now, before):
            totals = add(now[0], before[1])
            differs = add(couple(coef(5, w), coef(4, w), here[1]), sub(now[2], before[2]))
            for i in range(4):
                v = of(i, w)
                visit(i, w, v, ((totals[i] - differs[i]) + given(2, i, w) * v) + prev_k(totals[i] + differs[i]))

        wrapped = [next_z(of(i, 0)) for i in range(4)]
        turned = [next_k(v) for v in wrapped]
        nodes = [load(w) for w in range(16)] + [(add(wrapped, turned), sub(turned, wrapped))]
        made = {}
        for w in (*range(EARLY), 15, *range(EARLY, 15)):
            made[w] = column(w, nodes[w], nodes[w + 1])
            if w == 15:
                made[-1] = [[prev_z(v) for v in vs] for vs in made[15]]
                for early in range(EARLY):
                    finish(early, nodes[early], made[early], made[early - 1])
            elif w >= EARLY:
                finish(w, nodes[w], made[w], made[w - 1])
        finish(15, nodes[15], made[15], made[14])

    def over_all(v):
        return jnp.sum(jnp.sum(v, axis=1, keepdims=True), axis=0, keepdims=True)

    zero = jnp.zeros((8, 128), jnp.float32)

    crosses = [zero] * 4
    squares = [zero] * 4

    def measure(i, w, v, image):
        crosses[i] = crosses[i] + v * image
        squares[i] = squares[i] + image * image
        start_ref[i, w] = image

    apply(measure, lambda i, w: given(0, i, w), lambda i, w: next_k(given(0, i, w)))
    cross = over_all((crosses[0] + crosses[1]) + (crosses[2] + crosses[3]))
    square = over_all((squares[0] + squares[1]) + (squares[2] + squares[3]))
    per_theta = cross / square

    def advanced(step):
        kept, added = RHOS[1] * RHOS[0], 2.0 * RHOS[1] / HALF
        if not isinstance(step, int) or step:
            for n in range(1, DEGREE - 1):
                kept = jnp.where(step == n, RHOS[n + 1] * RHOS[n], kept)
                added = jnp.where(step == n, 2.0 * RHOS[n + 1] / HALF, added)
        return kept, jnp.broadcast_to(added * per_theta, (8, 128))

    start_of = lambda i, w: given(0, i, w)
    scale = jnp.broadcast_to(per_theta * (1.0 / CENTER), (8, 128))
    along, across = advanced(0)
    for i, w in cells:
        s = start_of(i, w)
        r = s - start_ref[i, w] * scale
        residual_ref[i, w] = r
        save(i, w, along * (s * scale) + across * r)
    for ij in range(8):
        correct_ref[ij] = parts_ref[lax.axis_index("core"), lax.axis_index("x"), 0, ij] * scale

    for sweep in range(SWEEPS):
        if sweep:
            for ij in range(8):
                correct_ref[ij] = zero
            for i, w in cells:
                residual_ref[i, w] = start_of(i, w)

        def correct():
            for ij in range(8):
                correct_ref[ij] = correct_ref[ij] + direct_ref[ij // 2, mine * 2 + ij % 2]

        def step(number, carry):
            correct()
            along, across = advanced(number)

            def advance(i, w, v, image):
                r = residual_ref[i, w] - image
                residual_ref[i, w] = r
                save(i, w, along * v + across * r)

            apply(advance)
            return carry

        lax.fori_loop(0 if sweep else 1, DEGREE - 1, step, 0)
        correct()
        crosses = [zero] * 4
        squares = [zero] * 4

        def finish_sweep(i, w, v, image):
            r = residual_ref[i, w] - image
            residual_ref[i, w] = r
            s = start_of(i, w)
            change = s - r
            crosses[i] = crosses[i] + s * change
            squares[i] = squares[i] + change * change

        apply(finish_sweep)
        along = over_all((crosses[0] + crosses[1]) + (crosses[2] + crosses[3]))
        length = over_all((squares[0] + squares[1]) + (squares[2] + squares[3]))
        omega = jnp.broadcast_to(along / length, (8, 128))
        squares = [zero] * 4
        for i, w in cells:
            s = start_of(i, w)
            r = s - omega * (s - residual_ref[i, w])
            squares[i] = squares[i] + r * r
            if sweep < SWEEPS - 1:
                start_ref[i, w] = r
                save(i, w, r * scale)
        start_of = lambda i, w: start_ref[i, w]
        total = over_all((squares[0] + squares[1]) + (squares[2] + squares[3]))
        rms = jnp.broadcast_to(jnp.sqrt(total / 65536.0), (8, 128))
        if sweep == 0:
            history = rms
            answer = [omega * correct_ref[ij] for ij in range(8)]
        else:
            history = jnp.where(lane == sweep, rms, history)
            answer = [a + omega * correct_ref[ij] for ij, a in enumerate(answer)]

    for y, tile in enumerate(exchange_rows(answer)):
        out_ref[y * 8 : y * 8 + 8, 0, 0:128] = exchange_lanes(tile)
        out_ref[y * 8 : y * 8 + 8, 0, 128:256] = history


def field(*lead):
    return pltpu.VMEM((*lead, 8, 128), jnp.float32)


def solve(parts):
    whole = field(4, 16)
    return pl.pallas_call(
        solve_kernel,
        out_shape=jax.ShapeDtypeStruct((64, 1, 256), jnp.float32),
        scratch_shapes=[
            whole, whole, whole, whole, field(6, 4, 16), field(8),
        ],
        compiler_params=SMALL,
        name="solve",
    )(parts)


def in_hbm(array):
    return pltpu.with_memory_space_constraint(array, pltpu.HBM)


def on_device(right_side, links, coefs, reaction):
    message, order = pl.pallas_call(
        pack_kernel,
        out_shape=(jax.ShapeDtypeStruct((64, 1, 384), jnp.float32), jax.ShapeDtypeStruct((128, 128), jnp.bfloat16)),
        in_specs=[pl.BlockSpec(memory_space=pltpu.HBM)] * 4,
        scratch_shapes=[
            pltpu.VMEM((64, 128), jnp.float32), pltpu.VMEM((8, 128), jnp.int32),
            pltpu.VMEM((1, 128), jnp.float32), pltpu.VMEM((1, 128), jnp.float32), pltpu.SemaphoreType.DMA((4,)),
        ],
        compiler_params=SMALL,
        name="pack",
    )(*(in_hbm(a) for a in (right_side, links, coefs.reshape(1, 128), reaction.reshape(1, 128))))
    received = lax.all_to_all(message, ("grp", "z"), 0, 0, tiled=True)
    spread = pl.pallas_call(
        spread_kernel,
        out_shape=jax.ShapeDtypeStruct((4, 3, 8, 8, 128), jnp.float32),
        compiler_params=SMALL,
        name="spread",
    )(received.reshape(64, 384))
    parts = lax.all_gather(lax.all_to_all(spread, "x", 0, 0, tiled=True), "core", axis=0)
    answer = solve(parts)
    answer = lax.all_to_all(answer, ("grp", "z"), 0, 0, tiled=True)
    return pl.pallas_call(
        unpack_kernel,
        out_shape=(jax.ShapeDtypeStruct((64, 128), jnp.float32), jax.ShapeDtypeStruct((SWEEPS, 64), jnp.float32)),
        compiler_params=SMALL,
        name="unpack",
    )(answer.reshape(64, 256), order)


def solution(mesh):
    finer = Mesh(mesh.devices.reshape(8, 8, 4, 2), ("grp", "z", "x", "core"))
    blocks = ("grp", "z", "x", "core")
    return jax.shard_map(
        on_device,
        mesh=finer,
        in_specs=(P(None, blocks), P(None, blocks), P(blocks), P(blocks)),
        out_specs=(P(None, blocks), P()),
        check_vma=False,
    )
```
